32 devices in a mesh: row: 8 (over z, y), col: 4 (over x, core).
Axes of the slice: x: 2, y: 2, z: 4, core: 2. Of those that a mesh axis runs over, the one named last changes fastest.
Arguments:
- right_side: float32 [3, 64, 512], P(None, 'row', 'col'), may hold values from -6 to 6
- viscosity: float32 [64, 512], P('row', 'col'), may hold values from 0.1 to 3
- free_mask: int32 [3, 64, 512], P(None, 'row', 'col'), may hold values 0 or 1
- coarse_basis: float32 [64, 3, 64, 512], P(None, None, 'row', 'col'), may hold values from -6 to 6
- gram_inverse: float32 [64, 64], P('col'), may hold values from -3 to 6, as said below
Outputs:
- solution: float32 [3, 64, 512], P(None, 'row', 'col')
- residual: float32 [3, 64, 512], P(None, 'row', 'col')
The draws below stay inside these ranges and needn't reach their ends.
Inputs may be any that keep to these rules, and one draw needn't show every extreme that they name: `free_mask`: 1 marks a free velocity unknown, 0 one whose value is prescribed. `gram_inverse`: symmetric positive definite.
All inputs are finite; a program needn't handle non-finite values. No bound on the sum of `free_mask` on one device may be relied on, other than what follows from the above.
Results may differ from the reference program's by a relative error of at most 0.0003.
Values sent between devices are 32-bit elements; how exact they have to be, the bound alone decides.
A program may use at most 64 MiB of HBM per device.

```python
import math
import jax
import jax.numpy as jnp
from jax import lax

COMP = 3
BASIS = 64
ITERS = 2
NA = 64
NB = 512


def draw_gram_inverse(key, part):
    base_key = jax.random.fold_in(key, 7)
    first_key, second_key = jax.random.split(base_key)
    factor = jax.random.uniform(first_key, (BASIS, BASIS), jnp.float32, -1.0, 1.0)
    square = jnp.dot(factor, factor.T, precision=lax.Precision.HIGHEST) * (3.0 / BASIS)
    square = 0.5 * (square + square.T)
    diagonal = jax.random.uniform(second_key, (BASIS,), jnp.float32, 1.0, 3.0)
    return (square + jnp.diag(diagonal)).astype(jnp.float32)


def set_ends(values, stream_key, smallest, largest):
    extent = values.shape
    spot = [jax.random.randint(jax.random.fold_in(stream_key, axis), (), 0, extent[axis]) for axis in range(len(extent))]
    values = values.at[tuple(spot)].set(smallest)
    longest = extent.index(max(extent))
    spot[longest] = (spot[longest] + 1) % extent[longest]
    return values.at[tuple(spot)].set(largest)


def steps_of(own_key, dims, shards, smallest, high):
    loudness = 1.0
    for dim, parts in shards:
        steps = jax.random.uniform(jax.random.fold_in(jax.random.fold_in(own_key, 6), dim), (parts,), jnp.float32, smallest / len(shards), high / len(shards))
        loudness = loudness * jnp.repeat(jnp.exp(steps), dims[dim] // parts).reshape((-1,) + (1,) * (len(dims) - 1 - dim))
    return loudness


def scatter_about(key, dims, width, most, cuts=(), kind=jnp.bfloat16):
    drawn = jax.random.normal(key, dims, jnp.float32) * width
    if len(cuts) > 0:
        drawn = steps_of(key, dims, cuts, -0.22, 0.18) * drawn
    return jnp.clip(drawn, min=-most, max=most).astype(kind)


def setup_inputs(seed: int = 0) -> dict:
    arg_keys = jax.random.split(jax.random.key(seed), 6)
    right_side = scatter_about(arg_keys[0], (COMP, NA, NB), 1.0, 6.0, ((1, 8), (2, 4)), jnp.float32)
    viscosity = jnp.clip(jnp.exp(math.log(3.0) - 3.4011974 * jax.random.uniform(arg_keys[1], (NA, NB), jnp.float32) ** steps_of(arg_keys[1], (NA, NB), ((0, 8), (1, 4)), -0.2, 0.2)), 0.1, 3.0)
    free_mask = set_ends((jax.random.randint(arg_keys[2], (COMP, NA, NB), 0, 8) < 7).astype(jnp.int32), jax.random.fold_in(arg_keys[2], 1), 0, 1)
    coarse_basis = scatter_about(arg_keys[3], (BASIS, COMP, NA, NB), 1.0, 6.0, ((2, 8), (3, 4)), jnp.float32)
    gram_inverse = draw_gram_inverse(jax.random.fold_in(arg_keys[5], 71), 0)
    return dict(right_side=right_side, viscosity=viscosity, free_mask=free_mask, coarse_basis=coarse_basis, gram_inverse=gram_inverse)


def face_terms(viscosity):
    padded = jnp.pad(viscosity, ((1, 1), (1, 1)))
    face_north = 0.5 * (viscosity + padded[2:, 1:-1])
    face_south = 0.5 * (viscosity + padded[:-2, 1:-1])
    face_east = 0.5 * (viscosity + padded[1:-1, 2:])
    face_west = 0.5 * (viscosity + padded[1:-1, :-2])
    diagonal = 1.0 + face_north + face_south + face_east + face_west
    return (face_north, face_south, face_east, face_west, diagonal)

def operate(vector, unfixed, faces):
    face_north, face_south, face_east, face_west, diagonal = faces
    masked = unfixed * vector
    padded = jnp.pad(masked, ((0, 0), (1, 1), (1, 1)))
    stencil = diagonal * masked - (face_north * padded[:, 2:, 1:-1] + face_south * padded[:, :-2, 1:-1] + face_east * padded[:, 1:-1, 2:] + face_west * padded[:, 1:-1, :-2])
    return unfixed * stencil + (1.0 - unfixed) * vector

def reference(right_side, viscosity, free_mask, coarse_basis, gram_inverse):
    high = lax.Precision.HIGHEST
    coarse_scale = 1.0 / (32.0 * math.sqrt(float(COMP * NA * NB * BASIS)))
    faces = face_terms(viscosity)
    unfixed = free_mask.astype(jnp.float32)
    jacobi = unfixed / faces[4] + (1.0 - unfixed)
    basis_rows = coarse_basis.reshape(BASIS, -1)

    def precondition(residual):
        coarse_dot = jnp.dot(basis_rows, residual.reshape(-1), precision=high)
        weighted_sq = jnp.sum(jacobi * residual * residual)
        coeffs = jnp.dot(gram_inverse, coarse_dot, precision=high) * coarse_scale
        smoothed = jacobi * residual + jnp.dot(coeffs, basis_rows, precision=high).reshape(residual.shape)
        return (smoothed, weighted_sq + jnp.dot(coarse_dot, coeffs, precision=high))
    solution = jnp.zeros_like(right_side)
    residual = right_side
    direction, energy = precondition(residual)
    for iteration in range(ITERS):
        applied = operate(direction, unfixed, faces)
        step_len = energy / jnp.sum(direction * applied)
        solution = solution + step_len * direction
        residual = residual - step_len * applied
        if iteration + 1 < ITERS:
            smoothed, energy_new = precondition(residual)
            direction = smoothed + energy_new / energy * direction
            energy = energy_new
    return (solution, residual)
```

```python
import functools
import math

import jax
import jax.numpy as jnp
from jax import lax
from jax.experimental import pallas as pl
from jax.experimental.pallas import tpu as pltpu
from jax.sharding import PartitionSpec as P

MESH = pl.DeviceIdType.MESH
HIGH = lax.Precision.HIGHEST
F32 = jnp.float32
OPPOSITE = (1, 0, 3, 2)


def zigzag(n):
    order = []
    for i in range(1, n // 2 + 1):
        order += [i, n - i] if 2 * i != n else [i]
    return order


def kernel(
    nrow,
    ncol,
    scale,
    r_hbm,
    visc_hbm,
    mask_hbm,
    basis_ref,
    gram_hbm,
    out_ref,
    r_ref,
    visc_ref,
    mask_ref,
    gram_ref,
    basis_t,
    row_recv,
    col_send,
    col_recv,
    edge_send,
    edge_recv,
    gram_full,
    sum_send,
    sum_recv,
    load_sem,
    small_sem,
    row_ssem,
    row_rsem,
    col_ssem,
    col_rsem,
    edge_ssem,
    edge_rsem,
    gram_ssem,
    gram_rsem,
    sum_ssem,
    sum_rsem,
):
    comps, rows, lanes = r_ref.shape
    basis = basis_ref.shape[0]
    cells = comps * rows
    n = nrow * ncol
    my_row, my_col = lax.axis_index("row"), lax.axis_index("col")
    me = my_row * ncol + my_col
    has = (my_row < nrow - 1, my_row > 0, my_col < ncol - 1, my_col > 0)
    where_to = (
        (my_row + 1, my_col),
        (my_row - 1, my_col),
        (my_row, my_col + 1),
        (my_row, my_col - 1),
    )

    loads = [
        pltpu.make_async_copy(
            basis_ref.at[:, c, r], basis_t.at[c, r], load_sem
        )
        for c in range(comps)
        for r in range(rows)
    ]
    small = [
        pltpu.make_async_copy(src, dst, small_sem.at[i])
        for i, (src, dst) in enumerate(
            (
                (r_hbm, r_ref),
                (visc_hbm, visc_ref),
                (mask_hbm, mask_ref),
                (gram_hbm, gram_ref),
            )
        )
    ]
    for load in small + loads:
        load.start()

    barrier = pltpu.get_barrier_semaphore()

    def to_all(act):
        def one(i, carry):
            t = lax.rem(me + i, n)
            act((t // ncol, lax.rem(t, ncol)))
            return carry

        if n <= 64:
            for i in zigzag(n):
                one(i, 0)
        else:
            lax.fori_loop(1, n, one, 0)

    to_all(
        lambda device: pl.semaphore_signal(
            barrier, inc=1, device_id=device, device_id_type=MESH
        )
    )

    for d in range(4):

        @pl.when(jnp.logical_not(has[d]))
        def _(d=d):
            for stage in range(3):
                edge_recv[stage, d] = jnp.zeros(edge_recv.shape[2:], F32)
            if d < 2:
                row_recv[d] = jnp.zeros(row_recv.shape[1:], F32)
            else:
                col_recv[d - 2] = jnp.zeros(col_recv.shape[1:], F32)

    lane_of = lax.broadcasted_iota(jnp.int32, (rows, lanes), 1)
    row_of = lax.broadcasted_iota(jnp.int32, (rows, lanes), 0)
    diag_mask = [lane_of == row_of + c * rows for c in range(comps)]
    wide_lane = lax.broadcasted_iota(jnp.int32, (basis, lanes), 1)

    def col_to_row(cols):
        out = None
        for c, col in enumerate(cols):
            term = jnp.sum(
                jnp.where(diag_mask[c], jnp.broadcast_to(col, (rows, lanes)), 0.0),
                axis=0,
                keepdims=True,
            )
            out = term if out is None else out + term
        return out

    def row_to_cols(row):
        wide = jnp.broadcast_to(row, (rows, lanes))
        return [
            jnp.sum(jnp.where(diag_mask[c], wide, 0.0), axis=1, keepdims=True)
            for c in range(comps)
        ]

    def shifted(x, north, south, east, west):
        return (
            jnp.where(row_of == rows - 1, north, pltpu.roll(x, rows - 1, axis=0)),
            jnp.where(row_of == 0, south, pltpu.roll(x, 1, axis=0)),
            jnp.where(lane_of == lanes - 1, east, pltpu.roll(x, lanes - 1, axis=1)),
            jnp.where(lane_of == 0, west, pltpu.roll(x, 1, axis=1)),
        )

    def edge_copy(stage, d):
        return pltpu.make_async_remote_copy(
            src_ref=edge_send.at[stage, d],
            dst_ref=edge_recv.at[stage, OPPOSITE[d]],
            send_sem=edge_ssem.at[stage, d],
            recv_sem=edge_rsem.at[stage, OPPOSITE[d]],
            device_id=where_to[d],
            device_id_type=MESH,
        )

    def edge_arrival(stage, d):
        return pltpu.make_async_remote_copy(
            src_ref=edge_send.at[stage, d],
            dst_ref=edge_recv.at[stage, d],
            send_sem=edge_ssem.at[stage, d],
            recv_sem=edge_rsem.at[stage, d],
            device_id=where_to[d],
            device_id_type=MESH,
        )

    def send_edges(stage):
        for d in range(4):
            pl.when(has[d])(edge_copy(stage, d).start)

    def wait_edges(stage):
        for d in range(4):
            pl.when(has[d])(edge_arrival(stage, d).wait_recv)

    def put_edge(stage, d, x, slot):
        if d < 2:
            at = rows - 1 if d == 0 else 0
            for c, part in enumerate(x):
                edge_send[stage, d, slot + c : slot + c + 1] = part[at : at + 1]
        else:
            at = lanes - 1 if d == 2 else 0
            edge_send[stage, d, slot : slot + 1] = col_to_row(
                [part[:, at : at + 1] for part in x]
            )

    def send_sums(phase, row):
        sum_send[phase] = row
        sum_recv[phase, me] = row

        to_all(
            lambda device: pltpu.make_async_remote_copy(
                src_ref=sum_send.at[phase],
                dst_ref=sum_recv.at[phase, me],
                send_sem=sum_ssem.at[phase],
                recv_sem=sum_rsem.at[phase],
                device_id=device,
                device_id_type=MESH,
            ).start()
        )

    def wait_sums(phase):
        others = sum_recv.at[phase, pl.ds(0, n - 1)]
        pltpu.make_async_copy(others, others, sum_rsem.at[phase]).wait()
        return jnp.sum(sum_recv[phase], axis=0)

    def total_row(blocks, sums):
        if sums:
            pad = jnp.zeros((rows - len(sums), lanes), F32)
            blocks = blocks + [jnp.concatenate(sums + [pad], axis=0)]
        out = None
        for i, block in enumerate(blocks):
            col = jnp.sum(block, axis=1, keepdims=True)
            term = jnp.where(lane_of == row_of + i * rows, col, 0.0)
            out = term if out is None else out + term
        return jnp.sum(out, axis=0, keepdims=True)

    def project(x):
        acc = None
        for c in range(comps):
            for r in range(rows):
                term = basis_t[c, r] * x[c][r : r + 1]
                acc = term if acc is None else acc + term
        return [acc[i : i + rows] for i in range(0, basis, rows)]

    def lift(block, coeffs):
        return jnp.sum(block * coeffs, axis=0, keepdims=True)

    def lift_all(coeffs):
        return [
            jnp.concatenate([lift(basis_t[c, r], coeffs) for r in range(rows)], axis=0)
            for c in range(comps)
        ]

    def inner(xs, ys):
        out = None
        for x, y in zip(xs, ys):
            term = jnp.sum(x * y, axis=0, keepdims=True)
            out = term if out is None else out + term
        return out

    for load in small:
        load.wait()
    gram_full[my_col] = gram_ref[...]
    right = [r_ref[c] for c in range(comps)]
    free = [mask_ref[c].astype(F32) for c in range(comps)]
    visc = visc_ref[...]
    for d in range(4):
        slots = (0, comps, 2 * comps) if d < 2 else (0, 1, 2)
        put_edge(0, d, [visc], slots[2])
        put_edge(0, d, right, slots[0])
        put_edge(0, d, free, slots[1])

    pltpu.make_async_copy(basis_t, basis_t, load_sem).wait()
    first = total_row(project(right), [])

    pl.semaphore_wait(barrier, n - 1)
    send_sums(0, first)
    send_edges(0)

    def row_copy(d, dst):
        return pltpu.make_async_remote_copy(
            src_ref=basis_t.at[:, rows - 1 if d == 0 else 0],
            dst_ref=row_recv.at[dst],
            send_sem=row_ssem.at[d],
            recv_sem=row_rsem.at[dst],
            device_id=where_to[d],
            device_id_type=MESH,
        )

    def col_copy(d, dst):
        return pltpu.make_async_remote_copy(
            src_ref=col_send.at[d - 2],
            dst_ref=col_recv.at[dst - 2],
            send_sem=col_ssem.at[d - 2],
            recv_sem=col_rsem.at[dst - 2],
            device_id=where_to[d],
            device_id_type=MESH,
        )

    for d in range(2):
        pl.when(has[d])(row_copy(d, OPPOSITE[d]).start)

    def gram_copy(i):
        return pltpu.make_async_remote_copy(
            src_ref=gram_ref,
            dst_ref=gram_full.at[my_col],
            send_sem=gram_ssem,
            recv_sem=gram_rsem,
            device_id=(my_row, lax.rem(my_col + i, ncol)),
            device_id_type=MESH,
        )

    for i in range(1, ncol):
        gram_copy(i).start()

    for d in (2, 3):
        at = lanes - 1 if d == 2 else 0
        gathered = jnp.zeros((basis, lanes), F32)
        for c in range(comps):
            for r in range(rows):
                spot = c * rows + r
                turned = pltpu.roll(basis_t[c, r], (spot - at) % lanes, axis=1)
                gathered = jnp.where(wide_lane == spot, turned, gathered)
        col_send[d - 2] = gathered
        pl.when(has[d])(col_copy(d, OPPOSITE[d]).start)

    wait_edges(0)
    visc_halo = [edge_recv[0, d, 2 * comps : 2 * comps + 1] for d in range(2)]
    for d in (2, 3):
        visc_halo.append(row_to_cols(edge_recv[0, d, 2:3])[0])
    faces = [0.5 * (visc + v) for v in shifted(visc, *visc_halo)]
    diagonal = 1.0 + faces[0] + faces[1] + faces[2] + faces[3]
    inverse = 1.0 / diagonal
    scaled = [u * inverse for u in free]
    jacobi = [s + (1.0 - u) for s, u in zip(scaled, free)]
    for d in range(4):
        put_edge(1, d, scaled, 0)
    send_edges(1)

    def operate(x, halo):
        out = []
        for c in range(comps):
            masked = free[c] * x[c]
            around = shifted(masked, *[halo[d][c] for d in range(4)])
            stencil = diagonal * masked - (
                faces[0] * around[0]
                + faces[1] * around[1]
                + faces[2] * around[2]
                + faces[3] * around[3]
            )
            out.append(free[c] * stencil + (1.0 - free[c]) * x[c])
        return out

    def halos(coeffs, step):
        out = []
        for d in range(4):
            if d < 2:
                rows_out = []
                for c in range(comps):
                    res = edge_recv[0, d, c : c + 1]
                    if step is not None:
                        res = res - step * edge_recv[2, d, c : c + 1]
                    rows_out.append(
                        edge_recv[1, d, c : c + 1] * res
                        + edge_recv[0, d, comps + c : comps + c + 1]
                        * lift(row_recv[d, c], coeffs)
                    )
                out.append(rows_out)
            else:
                res = edge_recv[0, d, 0:1]
                if step is not None:
                    res = res - step * edge_recv[2, d, 0:1]
                row = edge_recv[1, d, 0:1] * res + edge_recv[0, d, 1:2] * lift(
                    col_recv[d - 2], coeffs
                )
                out.append(row_to_cols(row))
        return out

    for d in range(4):
        if d < 2:
            pl.when(has[d])(row_copy(d, d).wait_recv)
        else:
            pl.when(has[d])(col_copy(d, d).wait_recv)
    others = gram_full.at[pl.ds(0, ncol - 1)]
    pltpu.make_async_copy(others, others, gram_rsem).wait()
    gram = gram_full[...].reshape(basis, basis)
    wait_edges(1)

    def solve(dot):
        return jnp.sum(gram * dot[:, :basis], axis=1, keepdims=True) * scale

    dot = wait_sums(0)
    coeffs = solve(dot)
    direction = [j * r + b for j, r, b in zip(jacobi, right, lift_all(coeffs))]
    image = operate(direction, halos(coeffs, None))
    for d in range(4):
        put_edge(2, d, image, 0)
    send_edges(2)
    second = total_row(
        project(image), [inner(right, direction), inner(direction, image)]
    )
    send_sums(1, second)
    wait_edges(2)
    sums = wait_sums(1)
    energy = sums[:, basis : basis + 1]
    curve = sums[:, basis + 1 : basis + 2]
    step = energy / curve
    residual = [r - step * w for r, w in zip(right, image)]
    coeffs = solve(dot - step * sums)
    smoothed = [j * r + b for j, r, b in zip(jacobi, residual, lift_all(coeffs))]
    smoothed_image = operate(smoothed, halos(coeffs, step))
    third = total_row(
        [],
        [
            inner(residual, smoothed),
            inner(smoothed, image),
            inner(smoothed, smoothed_image),
        ],
    )
    send_sums(2, third)
    sums = wait_sums(2)
    energy_new = sums[:, 0:1]
    ratio = energy_new / energy
    curve_new = sums[:, 2:3] + ratio * (2.0 * sums[:, 1:2] + ratio * curve)
    step_new = energy_new / curve_new
    for c in range(comps):
        out_ref[c] = step * direction[c] + step_new * (smoothed[c] + ratio * direction[c])
        out_ref[comps + c] = residual[c] - step_new * (smoothed_image[c] + ratio * image[c])

    for phase in range(3):
        sent = sum_recv.at[phase, pl.ds(0, n - 1)]
        pltpu.make_async_copy(sent, sent, sum_ssem.at[phase]).wait()
    others = gram_full.at[pl.ds(0, ncol - 1)]
    pltpu.make_async_copy(others, others, gram_ssem).wait()
    for d in range(4):
        for stage in range(3):
            pl.when(has[d])(edge_copy(stage, d).wait_send)
        if d < 2:
            pl.when(has[d])(row_copy(d, d).wait_send)
        else:
            pl.when(has[d])(col_copy(d, d).wait_send)


def on_device(nrow, ncol, right_side, viscosity, free_mask, coarse_basis, gram_inverse):
    comps, rows, lanes = right_side.shape
    basis = coarse_basis.shape[0]
    n = nrow * ncol
    unknowns = comps * rows * lanes * n * basis
    scale = 1.0 / (32.0 * math.sqrt(float(unknowns)))
    vmem = pl.BlockSpec(memory_space=pltpu.VMEM)
    dma = pltpu.SemaphoreType.DMA
    out = pl.pallas_call(
        functools.partial(kernel, nrow, ncol, scale),
        out_shape=pltpu.VMEM((2 * comps, rows, lanes), F32),
        in_specs=[pl.BlockSpec(memory_space=pltpu.HBM)] * 5,
        out_specs=vmem,
        scratch_shapes=[
            pltpu.VMEM(right_side.shape, F32),
            pltpu.VMEM(viscosity.shape, F32),
            pltpu.VMEM(free_mask.shape, free_mask.dtype),
            pltpu.VMEM(gram_inverse.shape, F32),
            pltpu.VMEM((comps, rows, basis, lanes), F32),
            pltpu.VMEM((2, comps, basis, lanes), F32),
            pltpu.VMEM((2, basis, lanes), F32),
            pltpu.VMEM((2, basis, lanes), F32),
            pltpu.VMEM((3, 4, 8, lanes), F32),
            pltpu.VMEM((3, 4, 8, lanes), F32),
            pltpu.VMEM((ncol,) + gram_inverse.shape, F32),
            pltpu.VMEM((3, 1, lanes), F32),
            pltpu.VMEM((3, n, 1, lanes), F32),
            dma,
            dma((4,)),
            dma((2,)),
            dma((2,)),
            dma((2,)),
            dma((2,)),
            dma((3, 4)),
            dma((3, 4)),
            dma,
            dma,
            dma((3,)),
            dma((3,)),
        ],
        compiler_params=pltpu.CompilerParams(
            collective_id=0, has_side_effects=True, vmem_limit_bytes=60_000_000
        ),
    )(right_side, viscosity, free_mask, coarse_basis, gram_inverse)
    return out[:comps], out[comps:]


def solution(mesh):
    in_specs = (
        P(None, "row", "col"),
        P("row", "col"),
        P(None, "row", "col"),
        P(None, None, "row", "col"),
        P("col", None),
    )
    out_specs = (P(None, "row", "col"), P(None, "row", "col"))
    return jax.shard_map(
        functools.partial(on_device, mesh.shape["row"], mesh.shape["col"]),
        mesh=mesh,
        in_specs=in_specs,
        out_specs=out_specs,
        check_vma=False,
    )
```

```python
import functools
import math

import jax
import jax.numpy as jnp
from jax import lax
from jax.experimental import pallas as pl
from jax.experimental.pallas import tpu as pltpu
from jax.sharding import PartitionSpec as P

MESH = pl.DeviceIdType.MESH
HIGH = lax.Precision.HIGHEST
F32 = jnp.float32
OPPOSITE = (1, 0, 3, 2)


def zigzag(n):
    order = []
    for i in range(1, n // 2 + 1):
        order += [i, n - i] if 2 * i != n else [i]
    return order


def plane_rows(nrow):
    return max(d for d in range(1, nrow + 1) if nrow % d == 0 and d * d <= nrow)


def kernel(
    nrow,
    ncol,
    scale,
    r_hbm,
    visc_hbm,
    mask_hbm,
    basis_ref,
    gram_hbm,
    out_ref,
    r_ref,
    visc_ref,
    mask_ref,
    gram_ref,
    basis_t,
    row_recv,
    col_send,
    col_recv,
    edge_send,
    edge_recv,
    gram_full,
    sum_send,
    sum_recv,
    load_sem,
    small_sem,
    row_ssem,
    row_rsem,
    col_ssem,
    col_rsem,
    edge_ssem,
    edge_rsem,
    gram_ssem,
    gram_rsem,
    sum_ssem,
    sum_rsem,
    chain_sem,
):
    comps, rows, lanes = r_ref.shape
    basis = basis_ref.shape[0]
    cells = comps * rows
    n = nrow * ncol
    my_row, my_col = lax.axis_index("row"), lax.axis_index("col")
    me = my_row * ncol + my_col
    has = (my_row < nrow - 1, my_row > 0, my_col < ncol - 1, my_col > 0)
    where_to = (
        (my_row + 1, my_col),
        (my_row - 1, my_col),
        (my_row, my_col + 1),
        (my_row, my_col - 1),
    )

    loads = [
        pltpu.make_async_copy(
            basis_ref.at[:, c, r], basis_t.at[c, r], load_sem
        )
        for c in range(comps)
        for r in range(rows)
    ]
    small = [
        pltpu.make_async_copy(src, dst, small_sem.at[i])
        for i, (src, dst) in enumerate(
            (
                (r_hbm, r_ref),
                (visc_hbm, visc_ref),
                (mask_hbm, mask_ref),
                (gram_hbm, gram_ref),
            )
        )
    ]
    for load in small + loads:
        load.start()

    barrier = pltpu.get_barrier_semaphore()

    def to_all(act):
        def one(i, carry):
            t = lax.rem(me + i, n)
            act((t // ncol, lax.rem(t, ncol)))
            return carry

        if n <= 64:
            for i in zigzag(n):
                one(i, 0)
        else:
            lax.fori_loop(1, n, one, 0)

    depth = plane_rows(nrow)
    planes = nrow // depth
    group = depth * ncol
    plane, spot_row = my_row // depth, lax.rem(my_row, depth)
    mine = spot_row * ncol + my_col
    above, below = plane < planes - 1, plane > 0

    def greet(device):
        pl.semaphore_signal(barrier, inc=1, device_id=device, device_id_type=MESH)

    greeted = group - 1
    near = [(above, depth), (below, -depth)]
    if depth > 1:
        near.append((jnp.logical_and(above, spot_row == depth - 1), 1))
        near.append((jnp.logical_and(below, spot_row == 0), -1))
    for there, step in near:
        greeted = greeted + jnp.where(there, 1, 0)
        pl.when(there)(functools.partial(greet, (my_row + step, my_col)))
    for i in zigzag(group):
        t = lax.rem(mine + i, group)
        greet((plane * depth + t // ncol, lax.rem(t, ncol)))

    def pass_on(way, has_from, has_to, step):
        pl.when(has_from)(lambda: pl.semaphore_wait(chain_sem.at[way], 1))
        pl.when(has_to)(
            lambda: pl.semaphore_signal(
                chain_sem.at[way],
                inc=1,
                device_id=(my_row + step, my_col),
                device_id_type=MESH,
            )
        )

    def pass_up():
        pass_on(0, below, above, depth)

    def pass_down():
        pass_on(1, above, below, -depth)

    for d in range(4):

        @pl.when(jnp.logical_not(has[d]))
        def _(d=d):
            for stage in range(3):
                edge_recv[stage, d] = jnp.zeros(edge_recv.shape[2:], F32)
            if d < 2:
                row_recv[d] = jnp.zeros(row_recv.shape[1:], F32)
            else:
                col_recv[d - 2] = jnp.zeros(col_recv.shape[1:], F32)

    lane_of = lax.broadcasted_iota(jnp.int32, (rows, lanes), 1)
    row_of = lax.broadcasted_iota(jnp.int32, (rows, lanes), 0)
    diag_mask = [lane_of == row_of + c * rows for c in range(comps)]
    wide_lane = lax.broadcasted_iota(jnp.int32, (basis, lanes), 1)

    def col_to_row(cols):
        out = None
        for c, col in enumerate(cols):
            term = jnp.sum(
                jnp.where(diag_mask[c], jnp.broadcast_to(col, (rows, lanes)), 0.0),
                axis=0,
                keepdims=True,
            )
            out = term if out is None else out + term
        return out

    def row_to_cols(row):
        wide = jnp.broadcast_to(row, (rows, lanes))
        return [
            jnp.sum(jnp.where(diag_mask[c], wide, 0.0), axis=1, keepdims=True)
            for c in range(comps)
        ]

    def shifted(x, north, south, east, west):
        return (
            jnp.where(row_of == rows - 1, north, pltpu.roll(x, rows - 1, axis=0)),
            jnp.where(row_of == 0, south, pltpu.roll(x, 1, axis=0)),
            jnp.where(lane_of == lanes - 1, east, pltpu.roll(x, lanes - 1, axis=1)),
            jnp.where(lane_of == 0, west, pltpu.roll(x, 1, axis=1)),
        )

    def edge_copy(stage, d):
        return pltpu.make_async_remote_copy(
            src_ref=edge_send.at[stage, d],
            dst_ref=edge_recv.at[stage, OPPOSITE[d]],
            send_sem=edge_ssem.at[stage, d],
            recv_sem=edge_rsem.at[stage, OPPOSITE[d]],
            device_id=where_to[d],
            device_id_type=MESH,
        )

    def edge_arrival(stage, d):
        return pltpu.make_async_remote_copy(
            src_ref=edge_send.at[stage, d],
            dst_ref=edge_recv.at[stage, d],
            send_sem=edge_ssem.at[stage, d],
            recv_sem=edge_rsem.at[stage, d],
            device_id=where_to[d],
            device_id_type=MESH,
        )

    def send_edges(stage):
        for d in range(4):
            pl.when(has[d])(edge_copy(stage, d).start)

    def wait_edges(stage):
        for d in range(4):
            pl.when(has[d])(edge_arrival(stage, d).wait_recv)

    def put_edge(stage, d, x, slot):
        if d < 2:
            at = rows - 1 if d == 0 else 0
            for c, part in enumerate(x):
                edge_send[stage, d, slot + c : slot + c + 1] = part[at : at + 1]
        else:
            at = lanes - 1 if d == 2 else 0
            edge_send[stage, d, slot : slot + 1] = col_to_row(
                [part[:, at : at + 1] for part in x]
            )

    def keep_sums(phase, row):
        sum_send[phase] = row
        sum_recv[phase, me] = row

    def send_sums(phase):
        to_all(
            lambda device: pltpu.make_async_remote_copy(
                src_ref=sum_send.at[phase],
                dst_ref=sum_recv.at[phase, me],
                send_sem=sum_ssem.at[phase],
                recv_sem=sum_rsem.at[phase],
                device_id=device,
                device_id_type=MESH,
            ).start()
        )

    def wait_sums(phase):
        others = sum_recv.at[phase, pl.ds(0, n - 1)]
        pltpu.make_async_copy(others, others, sum_rsem.at[phase]).wait()
        return jnp.sum(sum_recv[phase], axis=0)

    def total_row(blocks, sums):
        if sums:
            pad = jnp.zeros((rows - len(sums), lanes), F32)
            blocks = blocks + [jnp.concatenate(sums + [pad], axis=0)]
        out = None
        for i, block in enumerate(blocks):
            col = jnp.sum(block, axis=1, keepdims=True)
            term = jnp.where(lane_of == row_of + i * rows, col, 0.0)
            out = term if out is None else out + term
        return jnp.sum(out, axis=0, keepdims=True)

    def project(x):
        acc = None
        for c in range(comps):
            for r in range(rows):
                term = basis_t[c, r] * x[c][r : r + 1]
                acc = term if acc is None else acc + term
        return [acc[i : i + rows] for i in range(0, basis, rows)]

    def lift(block, coeffs):
        return jnp.sum(block * coeffs, axis=0, keepdims=True)

    def lift_all(coeffs):
        return [
            jnp.concatenate([lift(basis_t[c, r], coeffs) for r in range(rows)], axis=0)
            for c in range(comps)
        ]

    def inner(xs, ys):
        out = None
        for x, y in zip(xs, ys):
            term = jnp.sum(x * y, axis=0, keepdims=True)
            out = term if out is None else out + term
        return out

    for load in small:
        load.wait()
    gram_full[my_col] = gram_ref[...]
    right = [r_ref[c] for c in range(comps)]
    free = [mask_ref[c].astype(F32) for c in range(comps)]
    visc = visc_ref[...]
    for d in range(4):
        slots = (0, comps, 2 * comps) if d < 2 else (0, 1, 2)
        put_edge(0, d, [visc], slots[2])
        put_edge(0, d, right, slots[0])
        put_edge(0, d, free, slots[1])

    def row_copy(d, dst):
        return pltpu.make_async_remote_copy(
            src_ref=basis_t.at[:, rows - 1 if d == 0 else 0],
            dst_ref=row_recv.at[dst],
            send_sem=row_ssem.at[d],
            recv_sem=row_rsem.at[dst],
            device_id=where_to[d],
            device_id_type=MESH,
        )

    def col_copy(d, dst):
        return pltpu.make_async_remote_copy(
            src_ref=col_send.at[d - 2],
            dst_ref=col_recv.at[dst - 2],
            send_sem=col_ssem.at[d - 2],
            recv_sem=col_rsem.at[dst - 2],
            device_id=where_to[d],
            device_id_type=MESH,
        )

    def gram_copy(i):
        return pltpu.make_async_remote_copy(
            src_ref=gram_ref,
            dst_ref=gram_full.at[my_col],
            send_sem=gram_ssem,
            recv_sem=gram_rsem,
            device_id=(my_row, lax.rem(my_col + i, ncol)),
            device_id_type=MESH,
        )

    pl.semaphore_wait(barrier, greeted)
    send_edges(0)
    pltpu.make_async_copy(basis_t, basis_t, load_sem).wait()
    for d in range(2):
        pl.when(has[d])(row_copy(d, OPPOSITE[d]).start)
    keep_sums(0, total_row(project(right), []))

    @pl.when(below)
    def _():
        pl.when(jnp.logical_not(above))(pass_down)
        pass_up()
        pl.when(above)(pass_down)
        send_sums(0)

    pl.when(jnp.logical_not(below))(pass_up)
    for i in range(1, ncol):
        gram_copy(i).start()

    lows = highs = jnp.zeros((basis, lanes), F32)
    for c in range(comps):
        for r in range(rows):
            spot = c * rows + r
            turned = pltpu.roll(basis_t[c, r], spot + 1, axis=1)
            highs = jnp.where(wide_lane == spot, turned, highs)
            lows = jnp.where(wide_lane == spot + 1, turned, lows)
    col_send[0] = highs
    col_send[1] = pltpu.roll(lows, lanes - 1, axis=1)
    for d in (2, 3):
        pl.when(has[d])(col_copy(d, OPPOSITE[d]).start)

    wait_edges(0)
    visc_halo = [edge_recv[0, d, 2 * comps : 2 * comps + 1] for d in range(2)]
    for d in (2, 3):
        visc_halo.append(row_to_cols(edge_recv[0, d, 2:3])[0])
    faces = [0.5 * (visc + v) for v in shifted(visc, *visc_halo)]
    diagonal = 1.0 + faces[0] + faces[1] + faces[2] + faces[3]
    inverse = 1.0 / diagonal
    scaled = [u * inverse for u in free]
    jacobi = [s + (1.0 - u) for s, u in zip(scaled, free)]
    for d in range(4):
        put_edge(1, d, scaled, 0)
    send_edges(1)

    @pl.when(jnp.logical_not(below))
    def _():
        pass_down()
        send_sums(0)

    def operate(x, halo):
        out = []
        for c in range(comps):
            masked = free[c] * x[c]
            around = shifted(masked, *[halo[d][c] for d in range(4)])
            stencil = diagonal * masked - (
                faces[0] * around[0]
                + faces[1] * around[1]
                + faces[2] * around[2]
                + faces[3] * around[3]
            )
            out.append(free[c] * stencil + (1.0 - free[c]) * x[c])
        return out

    def halos(coeffs, step):
        out = []
        for d in range(4):
            if d < 2:
                rows_out = []
                for c in range(comps):
                    res = edge_recv[0, d, c : c + 1]
                    if step is not None:
                        res = res - step * edge_recv[2, d, c : c + 1]
                    rows_out.append(
                        edge_recv[1, d, c : c + 1] * res
                        + edge_recv[0, d, comps + c : comps + c + 1]
                        * lift(row_recv[d, c], coeffs)
                    )
                out.append(rows_out)
            else:
                res = edge_recv[0, d, 0:1]
                if step is not None:
                    res = res - step * edge_recv[2, d, 0:1]
                row = edge_recv[1, d, 0:1] * res + edge_recv[0, d, 1:2] * lift(
                    col_recv[d - 2], coeffs
                )
                out.append(row_to_cols(row))
        return out

    for d in range(4):
        if d < 2:
            pl.when(has[d])(row_copy(d, d).wait_recv)
        else:
            pl.when(has[d])(col_copy(d, d).wait_recv)
    others = gram_full.at[pl.ds(0, ncol - 1)]
    pltpu.make_async_copy(others, others, gram_rsem).wait()
    gram = gram_full[...].reshape(basis, basis)
    wait_edges(1)

    def solve(dot):
        return jnp.sum(gram * dot[:, :basis], axis=1, keepdims=True) * scale

    dot = wait_sums(0)
    coeffs = solve(dot)
    direction = [j * r + b for j, r, b in zip(jacobi, right, lift_all(coeffs))]
    image = operate(direction, halos(coeffs, None))
    for d in range(4):
        put_edge(2, d, image, 0)
    send_edges(2)
    second = total_row(
        project(image), [inner(right, direction), inner(direction, image)]
    )
    keep_sums(1, second)
    send_sums(1)
    wait_edges(2)
    sums = wait_sums(1)
    energy = sums[:, basis : basis + 1]
    curve = sums[:, basis + 1 : basis + 2]
    step = energy / curve
    residual = [r - step * w for r, w in zip(right, image)]
    coeffs = solve(dot - step * sums)
    smoothed = [j * r + b for j, r, b in zip(jacobi, residual, lift_all(coeffs))]
    smoothed_image = operate(smoothed, halos(coeffs, step))
    third = total_row(
        [],
        [
            inner(residual, smoothed),
            inner(smoothed, image),
            inner(smoothed, smoothed_image),
        ],
    )
    keep_sums(2, third)
    send_sums(2)
    sums = wait_sums(2)
    energy_new = sums[:, 0:1]
    ratio = energy_new / energy
    curve_new = sums[:, 2:3] + ratio * (2.0 * sums[:, 1:2] + ratio * curve)
    step_new = energy_new / curve_new
    for c in range(comps):
        out_ref[c] = step * direction[c] + step_new * (smoothed[c] + ratio * direction[c])
        out_ref[comps + c] = residual[c] - step_new * (smoothed_image[c] + ratio * image[c])

    for phase in range(3):
        sent = sum_recv.at[phase, pl.ds(0, n - 1)]
        pltpu.make_async_copy(sent, sent, sum_ssem.at[phase]).wait()
    others = gram_full.at[pl.ds(0, ncol - 1)]
    pltpu.make_async_copy(others, others, gram_ssem).wait()
    for d in range(4):
        for stage in range(3):
            pl.when(has[d])(edge_copy(stage, d).wait_send)
        if d < 2:
            pl.when(has[d])(row_copy(d, d).wait_send)
        else:
            pl.when(has[d])(col_copy(d, d).wait_send)


def on_device(nrow, ncol, right_side, viscosity, free_mask, coarse_basis, gram_inverse):
    comps, rows, lanes = right_side.shape
    basis = coarse_basis.shape[0]
    n = nrow * ncol
    unknowns = comps * rows * lanes * n * basis
    scale = 1.0 / (32.0 * math.sqrt(float(unknowns)))
    vmem = pl.BlockSpec(memory_space=pltpu.VMEM)
    dma = pltpu.SemaphoreType.DMA
    out = pl.pallas_call(
        functools.partial(kernel, nrow, ncol, scale),
        out_shape=pltpu.VMEM((2 * comps, rows, lanes), F32),
        in_specs=[pl.BlockSpec(memory_space=pltpu.HBM)] * 5,
        out_specs=vmem,
        scratch_shapes=[
            pltpu.VMEM(right_side.shape, F32),
            pltpu.VMEM(viscosity.shape, F32),
            pltpu.VMEM(free_mask.shape, free_mask.dtype),
            pltpu.VMEM(gram_inverse.shape, F32),
            pltpu.VMEM((comps, rows, basis, lanes), F32),
            pltpu.VMEM((2, comps, basis, lanes), F32),
            pltpu.VMEM((2, basis, lanes), F32),
            pltpu.VMEM((2, basis, lanes), F32),
            pltpu.VMEM((3, 4, 8, lanes), F32),
            pltpu.VMEM((3, 4, 8, lanes), F32),
            pltpu.VMEM((ncol,) + gram_inverse.shape, F32),
            pltpu.VMEM((3, 1, lanes), F32),
            pltpu.VMEM((3, n, 1, lanes), F32),
            dma,
            dma((4,)),
            dma((2,)),
            dma((2,)),
            dma((2,)),
            dma((2,)),
            dma((3, 4)),
            dma((3, 4)),
            dma,
            dma,
            dma((3,)),
            dma((3,)),
            pltpu.SemaphoreType.REGULAR((2,)),
        ],
        compiler_params=pltpu.CompilerParams(
            collective_id=0, has_side_effects=True, vmem_limit_bytes=60_000_000
        ),
    )(right_side, viscosity, free_mask, coarse_basis, gram_inverse)
    return out[:comps], out[comps:]


def solution(mesh):
    in_specs = (
        P(None, "row", "col"),
        P("row", "col"),
        P(None, "row", "col"),
        P(None, None, "row", "col"),
        P("col", None),
    )
    out_specs = (P(None, "row", "col"), P(None, "row", "col"))
    return jax.shard_map(
        functools.partial(on_device, mesh.shape["row"], mesh.shape["col"]),
        mesh=mesh,
        in_specs=in_specs,
        out_specs=out_specs,
        check_vma=False,
    )
```

```python
import functools
import math

import jax
import jax.numpy as jnp
from jax import lax
from jax.experimental import pallas as pl
from jax.experimental.pallas import tpu as pltpu
from jax.sharding import PartitionSpec as P

MESH = pl.DeviceIdType.MESH
HIGH = lax.Precision.HIGHEST
F32 = jnp.float32
OPPOSITE = (1, 0, 3, 2)
NORTH, SOUTH, EAST, WEST = range(4)
EVERY = (NORTH, SOUTH, EAST, WEST)


def zigzag(n):
    order = []
    for i in range(1, n // 2 + 1):
        order += [i, n - i] if 2 * i != n else [i]
    return order


def plane_rows(nrow):
    return max(d for d in range(1, nrow + 1) if nrow % d == 0 and d * d <= nrow)


def kernel(
    nrow,
    ncol,
    scale,
    r_hbm,
    visc_hbm,
    mask_hbm,
    basis_ref,
    gram_hbm,
    out_ref,
    r_ref,
    visc_ref,
    mask_ref,
    gram_ref,
    basis_t,
    row_recv,
    col_send,
    col_recv,
    edge_send,
    edge_recv,
    diag_send,
    diag_recv,
    gram_full,
    sum_send,
    sum_recv,
    load_sem,
    small_sem,
    row_ssem,
    row_rsem,
    col_ssem,
    col_rsem,
    edge_ssem,
    edge_rsem,
    diag_ssem,
    diag_rsem,
    gram_ssem,
    gram_rsem,
    sum_ssem,
    sum_rsem,
    chain_sem,
):
    comps, rows, lanes = r_ref.shape
    basis = basis_ref.shape[0]
    cells = comps * rows
    n = nrow * ncol
    my_row, my_col = lax.axis_index("row"), lax.axis_index("col")
    me = my_row * ncol + my_col
    has = (my_row < nrow - 1, my_row > 0, my_col < ncol - 1, my_col > 0)
    where_to = (
        (my_row + 1, my_col),
        (my_row - 1, my_col),
        (my_row, my_col + 1),
        (my_row, my_col - 1),
    )

    has_diag = (
        jnp.logical_and(has[NORTH], has[WEST]),
        jnp.logical_and(has[SOUTH], has[EAST]),
    )
    diag_to = ((my_row + 1, my_col - 1), (my_row - 1, my_col + 1))

    loads = [
        pltpu.make_async_copy(
            basis_ref.at[:, c, r], basis_t.at[c, r], load_sem
        )
        for c in range(comps)
        for r in range(rows)
    ]
    small = [
        pltpu.make_async_copy(src, dst, small_sem.at[i])
        for i, (src, dst) in enumerate(
            (
                (r_hbm, r_ref),
                (visc_hbm, visc_ref),
                (mask_hbm, mask_ref),
                (gram_hbm, gram_ref),
            )
        )
    ]
    for load in small + loads:
        load.start()

    barrier = pltpu.get_barrier_semaphore()

    def to_all(act):
        def one(i, carry):
            t = lax.rem(me + i, n)
            act((t // ncol, lax.rem(t, ncol)))
            return carry

        if n <= 64:
            for i in zigzag(n):
                one(i, 0)
        else:
            lax.fori_loop(1, n, one, 0)

    depth = plane_rows(nrow)
    planes = nrow // depth
    group = depth * ncol
    plane, spot_row = my_row // depth, lax.rem(my_row, depth)
    mine = spot_row * ncol + my_col
    above, below = plane < planes - 1, plane > 0

    def greet(device):
        pl.semaphore_signal(barrier, inc=1, device_id=device, device_id_type=MESH)

    cross_down = jnp.logical_and(below, spot_row == 0)
    cross_up = jnp.logical_and(above, spot_row == depth - 1)
    greeted = plane * group + group - 1 + jnp.where(cross_up, 1, 0)
    pl.when(cross_down)(functools.partial(greet, (my_row - 1, my_col)))

    def greet_higher(i, carry):
        t = (plane + 1) * group + i
        greet((t // ncol, lax.rem(t, ncol)))
        return carry

    lax.fori_loop(0, (planes - 1 - plane) * group, greet_higher, 0)
    for i in zigzag(group):
        t = lax.rem(mine + i, group)
        greet((plane * depth + t // ncol, lax.rem(t, ncol)))

    def tell_lower():
        def tell(q, carry):
            pl.semaphore_signal(
                chain_sem,
                inc=1,
                device_id=(q * depth + spot_row, my_col),
                device_id_type=MESH,
            )
            return carry

        lax.fori_loop(0, plane, tell, 0)

    def hear_higher():
        pl.when(above)(lambda: pl.semaphore_wait(chain_sem, planes - 1 - plane))

    top = jnp.logical_not(above)

    for d in range(4):

        @pl.when(jnp.logical_not(has[d]))
        def _(d=d):
            for stage in range(4):
                edge_recv[stage, d] = jnp.zeros(edge_recv.shape[2:], F32)
            if d == SOUTH:
                row_recv[...] = jnp.zeros(row_recv.shape, F32)
            if d == WEST:
                col_recv[...] = jnp.zeros(col_recv.shape, F32)

    for i in range(2):

        @pl.when(jnp.logical_not(has_diag[1 - i]))
        def _(i=i):
            diag_recv[i] = jnp.zeros(diag_recv.shape[1:], F32)

    lane_of = lax.broadcasted_iota(jnp.int32, (rows, lanes), 1)
    row_of = lax.broadcasted_iota(jnp.int32, (rows, lanes), 0)
    diag_mask = [lane_of == row_of + c * rows for c in range(comps)]
    wide_lane = lax.broadcasted_iota(jnp.int32, (basis, lanes), 1)

    def col_to_row(cols):
        out = None
        for c, col in enumerate(cols):
            term = jnp.sum(
                jnp.where(diag_mask[c], jnp.broadcast_to(col, (rows, lanes)), 0.0),
                axis=0,
                keepdims=True,
            )
            out = term if out is None else out + term
        return out

    def row_to_cols(row):
        wide = jnp.broadcast_to(row, (rows, lanes))
        return [
            jnp.sum(jnp.where(diag_mask[c], wide, 0.0), axis=1, keepdims=True)
            for c in range(comps)
        ]

    def shifted(x, north, south, east, west):
        return (
            jnp.where(row_of == rows - 1, north, pltpu.roll(x, rows - 1, axis=0)),
            jnp.where(row_of == 0, south, pltpu.roll(x, 1, axis=0)),
            jnp.where(lane_of == lanes - 1, east, pltpu.roll(x, lanes - 1, axis=1)),
            jnp.where(lane_of == 0, west, pltpu.roll(x, 1, axis=1)),
        )

    def edge_copy(stage, d):
        return pltpu.make_async_remote_copy(
            src_ref=edge_send.at[stage, d],
            dst_ref=edge_recv.at[stage, OPPOSITE[d]],
            send_sem=edge_ssem.at[stage, d],
            recv_sem=edge_rsem.at[stage, OPPOSITE[d]],
            device_id=where_to[d],
            device_id_type=MESH,
        )

    def edge_arrival(stage, d):
        return pltpu.make_async_remote_copy(
            src_ref=edge_send.at[stage, d],
            dst_ref=edge_recv.at[stage, d],
            send_sem=edge_ssem.at[stage, d],
            recv_sem=edge_rsem.at[stage, d],
            device_id=where_to[d],
            device_id_type=MESH,
        )

    def diag_copy(i):
        return pltpu.make_async_remote_copy(
            src_ref=diag_send.at[i],
            dst_ref=diag_recv.at[i],
            send_sem=diag_ssem.at[i],
            recv_sem=diag_rsem.at[i],
            device_id=diag_to[i],
            device_id_type=MESH,
        )

    def send_edges(stage, ways):
        for d in ways:
            pl.when(has[d])(edge_copy(stage, d).start)

    def wait_edges(stage, sides):
        for d in sides:
            pl.when(has[d])(edge_arrival(stage, d).wait_recv)

    def edge_rows(d, x):
        if d < 2:
            at = rows - 1 if d == NORTH else 0
            return [part[at : at + 1] for part in x]
        at = lanes - 1 if d == EAST else 0
        return [col_to_row([part[:, at : at + 1] for part in x])]

    def put_edge(stage, d, x, slot):
        for i, row in enumerate(edge_rows(d, x)):
            edge_send[stage, d, slot + i : slot + i + 1] = row

    def keep_sums(phase, row):
        sum_send[phase] = row
        sum_recv[phase, me] = row

    def send_sums(phase):
        to_all(
            lambda device: pltpu.make_async_remote_copy(
                src_ref=sum_send.at[phase],
                dst_ref=sum_recv.at[phase, me],
                send_sem=sum_ssem.at[phase],
                recv_sem=sum_rsem.at[phase],
                device_id=device,
                device_id_type=MESH,
            ).start()
        )

    def wait_sums(phase):
        others = sum_recv.at[phase, pl.ds(0, n - 1)]
        pltpu.make_async_copy(others, others, sum_rsem.at[phase]).wait()
        return jnp.sum(sum_recv[phase], axis=0)

    def total_row(blocks, sums):
        if sums:
            pad = jnp.zeros((rows - len(sums), lanes), F32)
            blocks = blocks + [jnp.concatenate(sums + [pad], axis=0)]
        out = None
        for i, block in enumerate(blocks):
            col = jnp.sum(block, axis=1, keepdims=True)
            term = jnp.where(lane_of == row_of + i * rows, col, 0.0)
            out = term if out is None else out + term
        return jnp.sum(out, axis=0, keepdims=True)

    def project(x):
        acc = None
        for c in range(comps):
            for r in range(rows):
                term = basis_t[c, r] * x[c][r : r + 1]
                acc = term if acc is None else acc + term
        return [acc[i : i + rows] for i in range(0, basis, rows)]

    def lift(block, coeffs):
        return jnp.sum(block * coeffs, axis=0, keepdims=True)

    def lift_all(coeffs):
        return [
            jnp.concatenate([lift(basis_t[c, r], coeffs) for r in range(rows)], axis=0)
            for c in range(comps)
        ]

    def inner(xs, ys):
        out = None
        for x, y in zip(xs, ys):
            term = jnp.sum(x * y, axis=0, keepdims=True)
            out = term if out is None else out + term
        return out

    for load in small:
        load.wait()
    gram_full[my_col] = gram_ref[...]
    right = [r_ref[c] for c in range(comps)]
    free = [mask_ref[c].astype(F32) for c in range(comps)]
    visc = visc_ref[...]
    for d in EVERY:
        put_edge(0, d, [visc], 2 * comps if d < 2 else 2)
    for d in (NORTH, EAST):
        put_edge(0, d, right, 0)
        put_edge(0, d, free, comps if d < 2 else 1)

    row_copy = pltpu.make_async_remote_copy(
        src_ref=basis_t.at[:, rows - 1],
        dst_ref=row_recv,
        send_sem=row_ssem,
        recv_sem=row_rsem,
        device_id=where_to[NORTH],
        device_id_type=MESH,
    )
    col_copy = pltpu.make_async_remote_copy(
        src_ref=col_send,
        dst_ref=col_recv,
        send_sem=col_ssem,
        recv_sem=col_rsem,
        device_id=where_to[EAST],
        device_id_type=MESH,
    )

    def gram_copy(i):
        return pltpu.make_async_remote_copy(
            src_ref=gram_ref,
            dst_ref=gram_full.at[my_col],
            send_sem=gram_ssem,
            recv_sem=gram_rsem,
            device_id=(my_row, lax.rem(my_col + i, ncol)),
            device_id_type=MESH,
        )

    pl.semaphore_wait(barrier, greeted)
    tell_lower()
    send_edges(0, EVERY)
    pltpu.make_async_copy(basis_t, basis_t, load_sem).wait()
    pl.when(has[NORTH])(row_copy.start)
    keep_sums(0, total_row(project(right), []))

    pl.when(top)(lambda: send_sums(0))
    for i in range(1, ncol):
        gram_copy(i).start()

    column = jnp.zeros((basis, lanes), F32)
    for c in range(comps):
        for r in range(rows):
            spot = c * rows + r
            turned = pltpu.roll(basis_t[c, r], (spot + 1) % lanes, axis=1)
            column = jnp.where(wide_lane == spot, turned, column)
    col_send[...] = column
    pl.when(has[EAST])(col_copy.start)

    def hear_and_send():
        hear_higher()
        send_sums(0)

    pl.when(above)(hear_and_send)

    wait_edges(0, EVERY)
    visc_halo = [edge_recv[0, d, 2 * comps : 2 * comps + 1] for d in range(2)]
    for d in (EAST, WEST):
        visc_halo.append(row_to_cols(edge_recv[0, d, 2:3])[0])
    faces = [0.5 * (visc + v) for v in shifted(visc, *visc_halo)]
    diagonal = 1.0 + faces[0] + faces[1] + faces[2] + faces[3]
    inverse = 1.0 / diagonal
    scaled = [u * inverse for u in free]
    jacobi = [s + (1.0 - u) for s, u in zip(scaled, free)]
    for d in (NORTH, EAST):
        put_edge(1, d, scaled, 0)
    send_edges(1, (NORTH, EAST))

    pl.when(has[SOUTH])(row_copy.wait_recv)
    pl.when(has[WEST])(col_copy.wait_recv)
    others = gram_full.at[pl.ds(0, ncol - 1)]
    pltpu.make_async_copy(others, others, gram_rsem).wait()
    gram = gram_full[...].reshape(basis, basis)
    wait_edges(1, (SOUTH, WEST))
    south_right = [edge_recv[0, SOUTH, c : c + 1] for c in range(comps)]
    south_free = [edge_recv[0, SOUTH, comps + c : comps + c + 1] for c in range(comps)]
    south_scaled = [edge_recv[1, SOUTH, c : c + 1] for c in range(comps)]
    west_right, west_free = edge_recv[0, WEST, 0:1], edge_recv[0, WEST, 1:2]
    west_scaled = edge_recv[1, WEST, 0:1]

    def operate(x, coeffs, south_res, west_res):
        south = [
            s * r + u * lift(row_recv[c], coeffs)
            for c, (s, r, u) in enumerate(zip(south_scaled, south_res, south_free))
        ]
        west = west_scaled * west_res + west_free * lift(col_recv[...], coeffs)
        west_cols = row_to_cols(west)
        out, to_south, to_west = [], [], []
        for c in range(comps):
            masked = free[c] * x[c]
            around = shifted(masked, 0.0, south[c], 0.0, west_cols[c])
            stencil = diagonal * masked - (
                faces[0] * around[0]
                + faces[1] * around[1]
                + faces[2] * around[2]
                + faces[3] * around[3]
            )
            out.append(free[c] * stencil + (1.0 - free[c]) * x[c])
            to_south.append(faces[1] * masked)
            to_west.append(faces[3] * masked)
        return out, to_south, to_west, south, west

    def put_terms(stage, to_south, to_west):
        south_rows = edge_rows(SOUTH, to_south)
        west_row = edge_rows(WEST, to_west)[0]
        for c in range(comps):
            edge_send[stage, SOUTH, c : c + 1] = south_rows[c]
        edge_send[stage, WEST, 0:1] = west_row
        return [-u * q for u, q in zip(south_free, south_rows)], -west_free * west_row

    def cross(south, west, south_term, west_term):
        total = west * west_term
        for a, b in zip(south, south_term):
            total = total + a * b
        return total

    def complete(stage, image):
        east_cols = row_to_cols(edge_recv[stage, EAST, 0:1])
        return [
            image[c]
            - free[c]
            * (
                jnp.where(row_of == rows - 1, edge_recv[stage, NORTH, c : c + 1], 0.0)
                + jnp.where(lane_of == lanes - 1, east_cols[c], 0.0)
            )
            for c in range(comps)
        ]

    def solve(dot):
        return jnp.sum(gram * dot[:, :basis], axis=1, keepdims=True) * scale

    dot = wait_sums(0)
    coeffs = solve(dot)
    direction = [j * r + b for j, r, b in zip(jacobi, right, lift_all(coeffs))]
    image, to_south, to_west, south, west = operate(
        direction, coeffs, south_right, west_right
    )
    south_term, west_term = put_terms(2, to_south, to_west)
    across = project(image)
    extra = col_recv[...] * west_term
    for c in range(comps):
        extra = extra + row_recv[c] * south_term[c]
    across = [a + extra[i * rows : (i + 1) * rows] for i, a in enumerate(across)]
    second = total_row(
        across,
        [
            inner(right, direction),
            inner(direction, image) + cross(south, west, south_term, west_term),
        ],
    )
    keep_sums(1, second)
    send_sums(1)
    for d in (NORTH, EAST):
        put_edge(2, d, image, 0)
    corner_row = jnp.where(row_of == rows - 1, 1.0, 0.0)
    turned = [pltpu.roll(q, lanes - 1, axis=1) for q in to_west]
    for c in range(comps):
        diag_send[0, c : c + 1] = jnp.where(
            lane_of == lanes - 1, turned[c], 0.0
        )[rows - 1 : rows]
    turned = [pltpu.roll(q, rows - 1, axis=0) * corner_row for q in to_south]
    diag_send[1, 0:1] = col_to_row([q[:, lanes - 1 : lanes] for q in turned])
    send_edges(2, EVERY)
    for i in range(2):
        pl.when(has_diag[i])(diag_copy(i).start)
    wait_edges(2, EVERY)
    for i in range(2):
        pl.when(has_diag[1 - i])(diag_copy(i).wait_recv)
    image = complete(2, image)
    south_image = [
        edge_recv[2, SOUTH, c : c + 1]
        + south_term[c]
        - south_free[c] * diag_recv[0, c : c + 1]
        for c in range(comps)
    ]
    west_image = edge_recv[2, WEST, 0:1] + west_term - west_free * diag_recv[1, 0:1]
    sums = wait_sums(1)
    energy = sums[:, basis : basis + 1]
    curve = sums[:, basis + 1 : basis + 2]
    step = energy / curve
    residual = [r - step * w for r, w in zip(right, image)]
    coeffs = solve(dot - step * sums)
    smoothed = [j * r + b for j, r, b in zip(jacobi, residual, lift_all(coeffs))]
    smoothed_image, to_south, to_west, south, west = operate(
        smoothed,
        coeffs,
        [r - step * w for r, w in zip(south_right, south_image)],
        west_right - step * west_image,
    )
    south_term, west_term = put_terms(3, to_south, to_west)
    third = total_row(
        [],
        [
            inner(residual, smoothed),
            inner(smoothed, image),
            inner(smoothed, smoothed_image)
            + cross(south, west, south_term, west_term),
        ],
    )
    keep_sums(2, third)
    send_sums(2)
    send_edges(3, (SOUTH, WEST))
    wait_edges(3, (NORTH, EAST))
    smoothed_image = complete(3, smoothed_image)
    sums = wait_sums(2)
    energy_new = sums[:, 0:1]
    ratio = energy_new / energy
    curve_new = sums[:, 2:3] + ratio * (2.0 * sums[:, 1:2] + ratio * curve)
    step_new = energy_new / curve_new
    for c in range(comps):
        out_ref[c] = step * direction[c] + step_new * (smoothed[c] + ratio * direction[c])
        out_ref[comps + c] = residual[c] - step_new * (smoothed_image[c] + ratio * image[c])

    for phase in range(3):
        sent = sum_recv.at[phase, pl.ds(0, n - 1)]
        pltpu.make_async_copy(sent, sent, sum_ssem.at[phase]).wait()
    others = gram_full.at[pl.ds(0, ncol - 1)]
    pltpu.make_async_copy(others, others, gram_ssem).wait()
    for stage, ways in enumerate((EVERY, (NORTH, EAST), EVERY, (SOUTH, WEST))):
        for d in ways:
            pl.when(has[d])(edge_copy(stage, d).wait_send)
    for i in range(2):
        pl.when(has_diag[i])(diag_copy(i).wait_send)
    pl.when(has[NORTH])(row_copy.wait_send)
    pl.when(has[EAST])(col_copy.wait_send)


def on_device(nrow, ncol, right_side, viscosity, free_mask, coarse_basis, gram_inverse):
    comps, rows, lanes = right_side.shape
    basis = coarse_basis.shape[0]
    n = nrow * ncol
    unknowns = comps * rows * lanes * n * basis
    scale = 1.0 / (32.0 * math.sqrt(float(unknowns)))
    vmem = pl.BlockSpec(memory_space=pltpu.VMEM)
    dma = pltpu.SemaphoreType.DMA
    out = pl.pallas_call(
        functools.partial(kernel, nrow, ncol, scale),
        out_shape=pltpu.VMEM((2 * comps, rows, lanes), F32),
        in_specs=[pl.BlockSpec(memory_space=pltpu.HBM)] * 5,
        out_specs=vmem,
        scratch_shapes=[
            pltpu.VMEM(right_side.shape, F32),
            pltpu.VMEM(viscosity.shape, F32),
            pltpu.VMEM(free_mask.shape, free_mask.dtype),
            pltpu.VMEM(gram_inverse.shape, F32),
            pltpu.VMEM((comps, rows, basis, lanes), F32),
            pltpu.VMEM((comps, basis, lanes), F32),
            pltpu.VMEM((basis, lanes), F32),
            pltpu.VMEM((basis, lanes), F32),
            pltpu.VMEM((4, 4, 8, lanes), F32),
            pltpu.VMEM((4, 4, 8, lanes), F32),
            pltpu.VMEM((2, 8, lanes), F32),
            pltpu.VMEM((2, 8, lanes), F32),
            pltpu.VMEM((ncol,) + gram_inverse.shape, F32),
            pltpu.VMEM((3, 1, lanes), F32),
            pltpu.VMEM((3, n, 1, lanes), F32),
            dma,
            dma((4,)),
            dma,
            dma,
            dma,
            dma,
            dma((4, 4)),
            dma((4, 4)),
            dma((2,)),
            dma((2,)),
            dma,
            dma,
            dma((3,)),
            dma((3,)),
            pltpu.SemaphoreType.REGULAR,
        ],
        compiler_params=pltpu.CompilerParams(
            collective_id=0, has_side_effects=True, vmem_limit_bytes=60_000_000
        ),
    )(right_side, viscosity, free_mask, coarse_basis, gram_inverse)
    return out[:comps], out[comps:]


def solution(mesh):
    in_specs = (
        P(None, "row", "col"),
        P("row", "col"),
        P(None, "row", "col"),
        P(None, None, "row", "col"),
        P("col", None),
    )
    out_specs = (P(None, "row", "col"), P(None, "row", "col"))
    return jax.shard_map(
        functools.partial(on_device, mesh.shape["row"], mesh.shape["col"]),
        mesh=mesh,
        in_specs=in_specs,
        out_specs=out_specs,
        check_vma=False,
    )
```

```python
import functools
import math

import jax
import jax.numpy as jnp
from jax import lax
from jax.experimental import pallas as pl
from jax.experimental.pallas import tpu as pltpu
from jax.sharding import PartitionSpec as P

MESH = pl.DeviceIdType.MESH
HIGH = lax.Precision.HIGHEST
F32 = jnp.float32
OPPOSITE = (1, 0, 3, 2)
NORTH, SOUTH, EAST, WEST = range(4)
EVERY = (NORTH, SOUTH, EAST, WEST)
SENT = (EVERY, (NORTH, EAST), EVERY, (SOUTH, WEST))
SENT_AT = {}
for _stage, _ways in enumerate(SENT):
    for _way in _ways:
        SENT_AT[_stage, _way] = len(SENT_AT)


def zigzag(n):
    order = []
    for i in range(1, n // 2 + 1):
        order += [i, n - i] if 2 * i != n else [i]
    return order


def plane_rows(nrow):
    return max(d for d in range(1, nrow + 1) if nrow % d == 0 and d * d <= nrow)


def kernel(
    nrow,
    ncol,
    scale,
    r_hbm,
    visc_hbm,
    mask_hbm,
    basis_ref,
    gram_hbm,
    out_ref,
    r_ref,
    visc_ref,
    mask_ref,
    gram_ref,
    basis_t,
    row_recv,
    col_send,
    col_recv,
    edge_send,
    edge_recv,
    diag_send,
    diag_recv,
    gram_full,
    sum_send,
    sum_recv,
    load_sem,
    small_sem,
    row_ssem,
    row_rsem,
    col_ssem,
    col_rsem,
    edge_ssem,
    edge_rsem,
    diag_ssem,
    diag_rsem,
    gram_ssem,
    gram_rsem,
    sum_ssem,
    sum_rsem,
    chain_sem,
):
    comps, rows, lanes = r_ref.shape
    basis = basis_ref.shape[0]
    cells = comps * rows
    n = nrow * ncol
    my_row, my_col = lax.axis_index("row"), lax.axis_index("col")
    me = my_row * ncol + my_col
    has = (my_row < nrow - 1, my_row > 0, my_col < ncol - 1, my_col > 0)
    where_to = (
        (my_row + 1, my_col),
        (my_row - 1, my_col),
        (my_row, my_col + 1),
        (my_row, my_col - 1),
    )

    has_diag = (
        jnp.logical_and(has[NORTH], has[WEST]),
        jnp.logical_and(has[SOUTH], has[EAST]),
    )
    diag_to = ((my_row + 1, my_col - 1), (my_row - 1, my_col + 1))

    loads = [
        pltpu.make_async_copy(
            basis_ref.at[:, c, r], basis_t.at[c, r], load_sem
        )
        for c in range(comps)
        for r in range(rows)
    ]
    small = [
        pltpu.make_async_copy(src, dst, small_sem.at[i])
        for i, (src, dst) in enumerate(
            (
                (r_hbm, r_ref),
                (visc_hbm, visc_ref),
                (mask_hbm, mask_ref),
                (gram_hbm, gram_ref),
            )
        )
    ]
    for load in small + loads:
        load.start()

    barrier = pltpu.get_barrier_semaphore()

    def to_all(act):
        def one(i, carry):
            t = lax.rem(me + i, n)
            act((t // ncol, lax.rem(t, ncol)))
            return carry

        if n <= 64:
            for i in zigzag(n):
                one(i, 0)
        else:
            lax.fori_loop(1, n, one, 0)

    depth = plane_rows(nrow)
    planes = nrow // depth
    group = depth * ncol
    plane, spot_row = my_row // depth, lax.rem(my_row, depth)
    mine = spot_row * ncol + my_col
    above, below = plane < planes - 1, plane > 0

    def greet(device):
        pl.semaphore_signal(barrier, inc=1, device_id=device, device_id_type=MESH)

    cross_down = jnp.logical_and(below, spot_row == 0)
    cross_up = jnp.logical_and(above, spot_row == depth - 1)
    greeted = plane * group + group - 1 + jnp.where(cross_up, 1, 0)
    pl.when(cross_down)(functools.partial(greet, (my_row - 1, my_col)))

    def greet_higher(i, carry):
        t = (plane + 1) * group + i
        greet((t // ncol, lax.rem(t, ncol)))
        return carry

    lax.fori_loop(0, (planes - 1 - plane) * group, greet_higher, 0)
    for i in zigzag(group):
        t = lax.rem(mine + i, group)
        greet((plane * depth + t // ncol, lax.rem(t, ncol)))

    def tell_lower():
        def tell(q, carry):
            pl.semaphore_signal(
                chain_sem,
                inc=1,
                device_id=(q * depth + spot_row, my_col),
                device_id_type=MESH,
            )
            return carry

        lax.fori_loop(0, plane, tell, 0)

    def hear_higher():
        pl.when(above)(lambda: pl.semaphore_wait(chain_sem, planes - 1 - plane))

    top = jnp.logical_not(above)

    for d in range(4):

        @pl.when(jnp.logical_not(has[d]))
        def _(d=d):
            for stage in range(4):
                edge_recv[stage, d] = jnp.zeros(edge_recv.shape[2:], F32)
            if d == SOUTH:
                row_recv[...] = jnp.zeros(row_recv.shape, F32)
            if d == WEST:
                col_recv[...] = jnp.zeros(col_recv.shape, F32)

    for i in range(2):

        @pl.when(jnp.logical_not(has_diag[1 - i]))
        def _(i=i):
            diag_recv[i] = jnp.zeros(diag_recv.shape[1:], F32)

    lane_of = lax.broadcasted_iota(jnp.int32, (rows, lanes), 1)
    row_of = lax.broadcasted_iota(jnp.int32, (rows, lanes), 0)
    diag_mask = [lane_of == row_of + c * rows for c in range(comps)]
    wide_lane = lax.broadcasted_iota(jnp.int32, (basis, lanes), 1)

    def col_to_row(cols):
        out = None
        for c, col in enumerate(cols):
            term = jnp.sum(
                jnp.where(diag_mask[c], jnp.broadcast_to(col, (rows, lanes)), 0.0),
                axis=0,
                keepdims=True,
            )
            out = term if out is None else out + term
        return out

    def row_to_cols(row):
        wide = jnp.broadcast_to(row, (rows, lanes))
        return [
            jnp.sum(jnp.where(diag_mask[c], wide, 0.0), axis=1, keepdims=True)
            for c in range(comps)
        ]

    def shifted(x, north, south, east, west):
        return (
            jnp.where(row_of == rows - 1, north, pltpu.roll(x, rows - 1, axis=0)),
            jnp.where(row_of == 0, south, pltpu.roll(x, 1, axis=0)),
            jnp.where(lane_of == lanes - 1, east, pltpu.roll(x, lanes - 1, axis=1)),
            jnp.where(lane_of == 0, west, pltpu.roll(x, 1, axis=1)),
        )

    def edge_copy(stage, d):
        return pltpu.make_async_remote_copy(
            src_ref=edge_send.at[stage, d],
            dst_ref=edge_recv.at[stage, OPPOSITE[d]],
            send_sem=edge_ssem.at[SENT_AT[stage, d]],
            recv_sem=edge_rsem.at[SENT_AT[stage, d]],
            device_id=where_to[d],
            device_id_type=MESH,
        )

    def edge_arrival(stage, d):
        at = SENT_AT[stage, OPPOSITE[d]]
        return pltpu.make_async_remote_copy(
            src_ref=edge_send.at[stage, d],
            dst_ref=edge_recv.at[stage, d],
            send_sem=edge_ssem.at[at],
            recv_sem=edge_rsem.at[at],
            device_id=where_to[d],
            device_id_type=MESH,
        )

    def drain_sums(phase):
        sent = sum_recv.at[phase, pl.ds(0, n - 1)]
        pltpu.make_async_copy(sent, sent, sum_ssem.at[phase]).wait()

    def drain_edges(stage):
        for d in SENT[stage]:
            pl.when(has[d])(edge_copy(stage, d).wait_send)

    def diag_copy(i):
        return pltpu.make_async_remote_copy(
            src_ref=diag_send.at[i],
            dst_ref=diag_recv.at[i],
            send_sem=diag_ssem.at[i],
            recv_sem=diag_rsem.at[i],
            device_id=diag_to[i],
            device_id_type=MESH,
        )

    def send_edges(stage, ways):
        for d in ways:
            pl.when(has[d])(edge_copy(stage, d).start)

    def wait_edges(stage, sides):
        for d in sides:
            pl.when(has[d])(edge_arrival(stage, d).wait_recv)

    def edge_rows(d, x):
        if d < 2:
            at = rows - 1 if d == NORTH else 0
            return [part[at : at + 1] for part in x]
        at = lanes - 1 if d == EAST else 0
        return [col_to_row([part[:, at : at + 1] for part in x])]

    def put_edge(stage, d, x, slot):
        for i, row in enumerate(edge_rows(d, x)):
            edge_send[stage, d, slot + i : slot + i + 1] = row

    def keep_sums(phase, row):
        sum_send[phase] = row
        sum_recv[phase, me] = row

    def send_sums(phase):
        to_all(
            lambda device: pltpu.make_async_remote_copy(
                src_ref=sum_send.at[phase],
                dst_ref=sum_recv.at[phase, me],
                send_sem=sum_ssem.at[phase],
                recv_sem=sum_rsem.at[phase],
                device_id=device,
                device_id_type=MESH,
            ).start()
        )

    def wait_sums(phase):
        others = sum_recv.at[phase, pl.ds(0, n - 1)]
        pltpu.make_async_copy(others, others, sum_rsem.at[phase]).wait()
        if n > 64:
            return jnp.sum(sum_recv[phase], axis=0)
        parts = [sum_recv[phase, i] for i in range(n)]
        while len(parts) > 1:
            odd = parts[len(parts) // 2 * 2 :]
            parts = [a + b for a, b in zip(parts[::2], parts[1::2])] + odd
        return parts[0]

    def spread(row, at):
        return jnp.broadcast_to(row[:, at : at + 1], (1, lanes))

    def total_row(blocks, sums):
        if sums:
            pad = jnp.zeros((rows - len(sums), lanes), F32)
            blocks = blocks + [jnp.concatenate(sums + [pad], axis=0)]
        out = None
        for i, block in enumerate(blocks):
            col = jnp.sum(block, axis=1, keepdims=True)
            term = jnp.where(lane_of == row_of + i * rows, col, 0.0)
            out = term if out is None else out + term
        return jnp.sum(out, axis=0, keepdims=True)

    def project(x):
        acc = None
        for c in range(comps):
            for r in range(rows):
                term = basis_t[c, r] * x[c][r : r + 1]
                acc = term if acc is None else acc + term
        return [acc[i : i + rows] for i in range(0, basis, rows)]

    def lift(block, coeffs):
        return jnp.sum(block * coeffs, axis=0, keepdims=True)

    def lift_all(coeffs):
        return [
            jnp.concatenate([lift(basis_t[c, r], coeffs) for r in range(rows)], axis=0)
            for c in range(comps)
        ]

    def inner(xs, ys):
        out = None
        for x, y in zip(xs, ys):
            term = jnp.sum(x * y, axis=0, keepdims=True)
            out = term if out is None else out + term
        return out

    for load in small:
        load.wait()
    gram_full[my_col] = gram_ref[...]
    right = [r_ref[c] for c in range(comps)]
    free = [mask_ref[c].astype(F32) for c in range(comps)]
    visc = visc_ref[...]
    for d in EVERY:
        put_edge(0, d, [visc], 2 * comps if d < 2 else 2)
    for d in (NORTH, EAST):
        put_edge(0, d, right, 0)
        put_edge(0, d, free, comps if d < 2 else 1)

    row_copy = pltpu.make_async_remote_copy(
        src_ref=basis_t.at[:, rows - 1],
        dst_ref=row_recv,
        send_sem=row_ssem,
        recv_sem=row_rsem,
        device_id=where_to[NORTH],
        device_id_type=MESH,
    )
    col_copy = pltpu.make_async_remote_copy(
        src_ref=col_send,
        dst_ref=col_recv,
        send_sem=col_ssem,
        recv_sem=col_rsem,
        device_id=where_to[EAST],
        device_id_type=MESH,
    )

    def gram_copy(i):
        return pltpu.make_async_remote_copy(
            src_ref=gram_ref,
            dst_ref=gram_full.at[my_col],
            send_sem=gram_ssem,
            recv_sem=gram_rsem,
            device_id=(my_row, lax.rem(my_col + i, ncol)),
            device_id_type=MESH,
        )

    pl.semaphore_wait(barrier, greeted)
    tell_lower()
    send_edges(0, EVERY)
    pltpu.make_async_copy(basis_t, basis_t, load_sem).wait()
    pl.when(has[NORTH])(row_copy.start)
    keep_sums(0, total_row(project(right), []))

    pl.when(top)(lambda: send_sums(0))
    for i in range(1, ncol):
        gram_copy(i).start()

    column = jnp.zeros((basis, lanes), F32)
    for c in range(comps):
        for r in range(rows):
            spot = c * rows + r
            turned = pltpu.roll(basis_t[c, r], (spot + 1) % lanes, axis=1)
            column = jnp.where(wide_lane == spot, turned, column)
    col_send[...] = column
    pl.when(has[EAST])(col_copy.start)

    def hear_and_send():
        hear_higher()
        send_sums(0)

    pl.when(above)(hear_and_send)

    wait_edges(0, (EAST, WEST))
    sides = [row_to_cols(edge_recv[0, d, 2:3])[0] for d in (EAST, WEST)]
    _, below_visc, *beside = shifted(visc, 0.0, 0.0, *sides)
    open_north = 1.0 + 0.5 * (visc + below_visc)
    for v in beside:
        open_north = open_north + 0.5 * (visc + v)
    edge_send[1, NORTH, 0:1] = open_north[rows - 1 : rows]
    send_edges(1, (NORTH,))

    wait_edges(0, (NORTH, SOUTH))
    visc_halo = [edge_recv[0, d, 2 * comps : 2 * comps + 1] for d in (NORTH, SOUTH)]
    faces = [0.5 * (visc + v) for v in shifted(visc, *visc_halo, *sides)]
    diagonal = 1.0 + faces[0] + faces[1] + faces[2] + faces[3]
    inverse = 1.0 / diagonal
    scaled = [u * inverse for u in free]
    jacobi = [s + (1.0 - u) for s, u in zip(scaled, free)]
    put_edge(1, EAST, scaled, 0)
    send_edges(1, (EAST,))

    pl.when(has[SOUTH])(row_copy.wait_recv)
    pl.when(has[WEST])(col_copy.wait_recv)
    others = gram_full.at[pl.ds(0, ncol - 1)]
    pltpu.make_async_copy(others, others, gram_rsem).wait()
    gram = gram_full[...].reshape(basis, basis)
    wait_edges(1, (SOUTH, WEST))
    south_right = [edge_recv[0, SOUTH, c : c + 1] for c in range(comps)]
    south_free = [edge_recv[0, SOUTH, comps + c : comps + c + 1] for c in range(comps)]
    south_inverse = 1.0 / jnp.where(
        has[SOUTH], edge_recv[1, SOUTH, 0:1] + faces[1][0:1], 1.0
    )
    south_scaled = [u * south_inverse for u in south_free]
    west_right, west_free = edge_recv[0, WEST, 0:1], edge_recv[0, WEST, 1:2]
    west_scaled = edge_recv[1, WEST, 0:1]

    def halo_values(lifted, south_res, west_res):
        south = [
            a * r + u * b
            for a, r, u, b in zip(south_scaled, south_res, south_free, lifted[0])
        ]
        return south, west_scaled * west_res + west_free * lifted[1]

    def lift_halos(coeffs):
        south = [lift(row_recv[c], coeffs) for c in range(comps)]
        return south, lift(col_recv[...], coeffs)

    def operate(x, south, west):
        west_cols = row_to_cols(west)
        out, to_south, to_west = [], [], []
        for c in range(comps):
            masked = free[c] * x[c]
            around = shifted(masked, 0.0, south[c], 0.0, west_cols[c])
            stencil = diagonal * masked - (
                faces[0] * around[0]
                + faces[1] * around[1]
                + faces[2] * around[2]
                + faces[3] * around[3]
            )
            out.append(free[c] * stencil + (1.0 - free[c]) * x[c])
            to_south.append(faces[1] * masked)
            to_west.append(faces[3] * masked)
        return out, to_south, to_west

    def put_terms(stage, to_south, to_west):
        south_rows = edge_rows(SOUTH, to_south)
        west_row = edge_rows(WEST, to_west)[0]
        for c in range(comps):
            edge_send[stage, SOUTH, c : c + 1] = south_rows[c]
        edge_send[stage, WEST, 0:1] = west_row
        return [-u * q for u, q in zip(south_free, south_rows)], -west_free * west_row

    def cross(south, west, south_term, west_term):
        total = west * west_term
        for a, b in zip(south, south_term):
            total = total + a * b
        return total

    def complete(stage, image):
        east_cols = row_to_cols(edge_recv[stage, EAST, 0:1])
        return [
            image[c]
            - free[c]
            * (
                jnp.where(row_of == rows - 1, edge_recv[stage, NORTH, c : c + 1], 0.0)
                + jnp.where(lane_of == lanes - 1, east_cols[c], 0.0)
            )
            for c in range(comps)
        ]

    def solve(dot):
        return jnp.sum(gram * dot[:, :basis], axis=1, keepdims=True) * scale

    dot = wait_sums(0)
    coeffs = solve(dot)
    lifted, lifted_halos = lift_all(coeffs), lift_halos(coeffs)
    direction = [j * r + b for j, r, b in zip(jacobi, right, lifted)]
    south, west = halo_values(lifted_halos, south_right, west_right)
    image, to_south, to_west = operate(direction, south, west)
    south_term, west_term = put_terms(2, to_south, to_west)
    across = project(image)
    extra = col_recv[...] * west_term
    for c in range(comps):
        extra = extra + row_recv[c] * south_term[c]
    across = [a + extra[i * rows : (i + 1) * rows] for i, a in enumerate(across)]
    second = total_row(
        across,
        [
            inner(right, direction),
            inner(direction, image) + cross(south, west, south_term, west_term),
        ],
    )
    keep_sums(1, second)
    send_sums(1)
    for d in (NORTH, EAST):
        put_edge(2, d, image, 0)
    corner_row = jnp.where(row_of == rows - 1, 1.0, 0.0)
    turned = [pltpu.roll(q, lanes - 1, axis=1) for q in to_west]
    for c in range(comps):
        diag_send[0, c : c + 1] = jnp.where(
            lane_of == lanes - 1, turned[c], 0.0
        )[rows - 1 : rows]
    turned = [pltpu.roll(q, rows - 1, axis=0) * corner_row for q in to_south]
    diag_send[1, 0:1] = col_to_row([q[:, lanes - 1 : lanes] for q in turned])
    send_edges(2, EVERY)
    for i in range(2):
        pl.when(has_diag[i])(diag_copy(i).start)
    wait_edges(2, EVERY)
    for i in range(2):
        pl.when(has_diag[1 - i])(diag_copy(i).wait_recv)
    image = complete(2, image)
    south_image = [
        edge_recv[2, SOUTH, c : c + 1]
        + south_term[c]
        - south_free[c] * diag_recv[0, c : c + 1]
        for c in range(comps)
    ]
    west_image = edge_recv[2, WEST, 0:1] + west_term - west_free * diag_recv[1, 0:1]
    sums = wait_sums(1)
    energy, curve = spread(sums, basis), spread(sums, basis + 1)
    step = energy / curve
    coeffs = solve(sums)
    residual = [r - step * w for r, w in zip(right, image)]
    smoothed = [
        j * r + (b - step * l)
        for j, r, b, l in zip(jacobi, residual, lifted, lift_all(coeffs))
    ]
    south_lift, west_lift = lift_halos(coeffs)
    south, west = halo_values(
        (
            [b - step * l for b, l in zip(lifted_halos[0], south_lift)],
            lifted_halos[1] - step * west_lift,
        ),
        [r - step * w for r, w in zip(south_right, south_image)],
        west_right - step * west_image,
    )
    smoothed_image, to_south, to_west = operate(smoothed, south, west)
    south_term, west_term = put_terms(3, to_south, to_west)
    third = total_row(
        [],
        [
            inner(residual, smoothed),
            inner(smoothed, image),
            inner(smoothed, smoothed_image)
            + cross(south, west, south_term, west_term),
        ],
    )
    keep_sums(2, third)
    send_sums(2)
    send_edges(3, (SOUTH, WEST))
    wait_edges(3, (NORTH, EAST))
    smoothed_image = complete(3, smoothed_image)
    for phase in range(2):
        drain_sums(phase)
    for stage in range(3):
        drain_edges(stage)
    for i in range(2):
        pl.when(has_diag[i])(diag_copy(i).wait_send)
    pl.when(has[NORTH])(row_copy.wait_send)
    pl.when(has[EAST])(col_copy.wait_send)
    pltpu.make_async_copy(others, others, gram_ssem).wait()
    sums = wait_sums(2)
    energy_new = spread(sums, 0)
    ratio = energy_new / energy
    curve_new = spread(sums, 2) + ratio * (2.0 * spread(sums, 1) + ratio * curve)
    step_new = energy_new / curve_new
    for c in range(comps):
        out_ref[c] = step * direction[c] + step_new * (smoothed[c] + ratio * direction[c])
        out_ref[comps + c] = residual[c] - step_new * (smoothed_image[c] + ratio * image[c])

    drain_sums(2)
    drain_edges(3)


def on_device(nrow, ncol, right_side, viscosity, free_mask, coarse_basis, gram_inverse):
    comps, rows, lanes = right_side.shape
    basis = coarse_basis.shape[0]
    n = nrow * ncol
    unknowns = comps * rows * lanes * n * basis
    scale = 1.0 / (32.0 * math.sqrt(float(unknowns)))
    vmem = pl.BlockSpec(memory_space=pltpu.VMEM)
    dma = pltpu.SemaphoreType.DMA
    out = pl.pallas_call(
        functools.partial(kernel, nrow, ncol, scale),
        out_shape=pltpu.VMEM((2 * comps, rows, lanes), F32),
        in_specs=[pl.BlockSpec(memory_space=pltpu.HBM)] * 5,
        out_specs=vmem,
        scratch_shapes=[
            pltpu.VMEM(right_side.shape, F32),
            pltpu.VMEM(viscosity.shape, F32),
            pltpu.VMEM(free_mask.shape, free_mask.dtype),
            pltpu.VMEM(gram_inverse.shape, F32),
            pltpu.VMEM((comps, rows, basis, lanes), F32),
            pltpu.VMEM((comps, basis, lanes), F32),
            pltpu.VMEM((basis, lanes), F32),
            pltpu.VMEM((basis, lanes), F32),
            pltpu.VMEM((4, 4, 8, lanes), F32),
            pltpu.VMEM((4, 4, 8, lanes), F32),
            pltpu.VMEM((2, 8, lanes), F32),
            pltpu.VMEM((2, 8, lanes), F32),
            pltpu.VMEM((ncol,) + gram_inverse.shape, F32),
            pltpu.VMEM((3, 1, lanes), F32),
            pltpu.VMEM((3, n, 1, lanes), F32),
            dma,
            dma((4,)),
            dma,
            dma,
            dma,
            dma,
            dma((len(SENT_AT),)),
            dma((len(SENT_AT),)),
            dma((2,)),
            dma((2,)),
            dma,
            dma,
            dma((3,)),
            dma((3,)),
            pltpu.SemaphoreType.REGULAR,
        ],
        compiler_params=pltpu.CompilerParams(
            collective_id=0, has_side_effects=True, vmem_limit_bytes=60_000_000
        ),
    )(right_side, viscosity, free_mask, coarse_basis, gram_inverse)
    return out[:comps], out[comps:]


def solution(mesh):
    in_specs = (
        P(None, "row", "col"),
        P("row", "col"),
        P(None, "row", "col"),
        P(None, None, "row", "col"),
        P("col", None),
    )
    out_specs = (P(None, "row", "col"), P(None, "row", "col"))
    return jax.shard_map(
        functools.partial(on_device, mesh.shape["row"], mesh.shape["col"]),
        mesh=mesh,
        in_specs=in_specs,
        out_specs=out_specs,
        check_vma=False,
    )
```

```python
import functools
import math

import jax
import jax.numpy as jnp
from jax import lax
from jax.experimental import pallas as pl
from jax.experimental.pallas import tpu as pltpu
from jax.sharding import PartitionSpec as P

MESH = pl.DeviceIdType.MESH
HIGH = lax.Precision.HIGHEST
F32 = jnp.float32
OPPOSITE = (1, 0, 3, 2)
NORTH, SOUTH, EAST, WEST = range(4)
EVERY = (NORTH, SOUTH, EAST, WEST)
SENT = (EVERY, (NORTH, EAST), EVERY, (SOUTH, WEST))
SENT_AT = {}
for _stage, _ways in enumerate(SENT):
    for _way in _ways:
        SENT_AT[_stage, _way] = len(SENT_AT)


def zigzag(n):
    order = []
    for i in range(1, n // 2 + 1):
        order += [i, n - i] if 2 * i != n else [i]
    return order


def plane_rows(nrow):
    return max(d for d in range(1, nrow + 1) if nrow % d == 0 and d * d <= nrow)


def kernel(
    nrow,
    ncol,
    scale,
    r_hbm,
    visc_hbm,
    mask_hbm,
    basis_ref,
    gram_hbm,
    out_ref,
    r_ref,
    visc_ref,
    mask_ref,
    gram_ref,
    basis_t,
    row_recv,
    col_send,
    col_recv,
    edge_send,
    edge_recv,
    diag_send,
    diag_recv,
    gram_full,
    sum_send,
    sum_recv,
    load_sem,
    small_sem,
    row_ssem,
    row_rsem,
    col_ssem,
    col_rsem,
    edge_ssem,
    edge_rsem,
    diag_ssem,
    diag_rsem,
    gram_ssem,
    gram_rsem,
    sum_ssem,
    sum_rsem,
    chain_sem,
):
    comps, rows, lanes = r_ref.shape
    basis = basis_ref.shape[0]
    cells = comps * rows
    n = nrow * ncol
    my_row, my_col = lax.axis_index("row"), lax.axis_index("col")
    me = my_row * ncol + my_col
    has = (my_row < nrow - 1, my_row > 0, my_col < ncol - 1, my_col > 0)
    where_to = (
        (my_row + 1, my_col),
        (my_row - 1, my_col),
        (my_row, my_col + 1),
        (my_row, my_col - 1),
    )

    has_diag = (
        jnp.logical_and(has[NORTH], has[WEST]),
        jnp.logical_and(has[SOUTH], has[EAST]),
    )
    diag_to = ((my_row + 1, my_col - 1), (my_row - 1, my_col + 1))

    loads = [
        pltpu.make_async_copy(
            basis_ref.at[:, c, r], basis_t.at[c, r], load_sem
        )
        for c in range(comps)
        for r in range(rows)
    ]
    small = [
        pltpu.make_async_copy(src, dst, small_sem.at[i])
        for i, (src, dst) in enumerate(
            (
                (r_hbm, r_ref),
                (visc_hbm, visc_ref),
                (mask_hbm, mask_ref),
                (gram_hbm, gram_ref),
            )
        )
    ]
    for load in small + loads:
        load.start()

    barrier = pltpu.get_barrier_semaphore()

    def target(dr, dc):
        return lax.rem(my_row + dr, nrow), lax.rem(my_col + dc, ncol)

    def to_all(act):
        if n <= 64:
            rows_to = [lax.rem(my_row + dr, nrow) for dr in range(nrow)]
            cols_to = [lax.rem(my_col + dc, ncol) for dc in range(ncol)]
            for dr in zigzag(nrow) + [0]:
                for dc in zigzag(ncol) + [0]:
                    if dr or dc:
                        act((rows_to[dr], cols_to[dc]))
            return

        def one(i, carry):
            t = lax.rem(me + i, n)
            act((t // ncol, lax.rem(t, ncol)))
            return carry

        lax.fori_loop(1, n, one, 0)

    depth = plane_rows(nrow)
    planes = nrow // depth
    group = depth * ncol
    plane, spot_row = my_row // depth, lax.rem(my_row, depth)
    mine = spot_row * ncol + my_col
    above, below = plane < planes - 1, plane > 0

    def greet(device):
        pl.semaphore_signal(barrier, inc=1, device_id=device, device_id_type=MESH)

    cross_down = jnp.logical_and(below, spot_row == 0)
    cross_up = jnp.logical_and(above, spot_row == depth - 1)
    greeted = plane * group + group - 1 + jnp.where(cross_up, 1, 0)
    pl.when(cross_down)(functools.partial(greet, (my_row - 1, my_col)))

    def greet_higher(i, carry):
        t = (plane + 1) * group + i
        greet((t // ncol, lax.rem(t, ncol)))
        return carry

    lax.fori_loop(0, (planes - 1 - plane) * group, greet_higher, 0)
    for i in zigzag(group):
        t = lax.rem(mine + i, group)
        greet((plane * depth + t // ncol, lax.rem(t, ncol)))

    def tell_lower():
        def tell(q, carry):
            pl.semaphore_signal(
                chain_sem,
                inc=1,
                device_id=(q * depth + spot_row, my_col),
                device_id_type=MESH,
            )
            return carry

        lax.fori_loop(0, plane, tell, 0)

    def hear_higher():
        pl.when(above)(lambda: pl.semaphore_wait(chain_sem, planes - 1 - plane))

    top = jnp.logical_not(above)

    for d in range(4):

        @pl.when(jnp.logical_not(has[d]))
        def _(d=d):
            for stage in range(4):
                edge_recv[stage, d] = jnp.zeros(edge_recv.shape[2:], F32)
            if d == SOUTH:
                row_recv[...] = jnp.zeros(row_recv.shape, F32)
            if d == WEST:
                col_recv[...] = jnp.zeros(col_recv.shape, F32)

    for i in range(2):

        @pl.when(jnp.logical_not(has_diag[1 - i]))
        def _(i=i):
            diag_recv[i] = jnp.zeros(diag_recv.shape[1:], F32)

    lane_of = lax.broadcasted_iota(jnp.int32, (rows, lanes), 1)
    row_of = lax.broadcasted_iota(jnp.int32, (rows, lanes), 0)
    diag_mask = [lane_of == row_of + c * rows for c in range(comps)]
    wide_lane = lax.broadcasted_iota(jnp.int32, (basis, lanes), 1)

    def col_to_row(cols):
        out = None
        for c, col in enumerate(cols):
            term = jnp.sum(
                jnp.where(diag_mask[c], jnp.broadcast_to(col, (rows, lanes)), 0.0),
                axis=0,
                keepdims=True,
            )
            out = term if out is None else out + term
        return out

    def row_to_cols(row):
        wide = jnp.broadcast_to(row, (rows, lanes))
        return [
            jnp.sum(jnp.where(diag_mask[c], wide, 0.0), axis=1, keepdims=True)
            for c in range(comps)
        ]

    def shifted(x, north, south, east, west):
        return (
            jnp.where(row_of == rows - 1, north, pltpu.roll(x, rows - 1, axis=0)),
            jnp.where(row_of == 0, south, pltpu.roll(x, 1, axis=0)),
            jnp.where(lane_of == lanes - 1, east, pltpu.roll(x, lanes - 1, axis=1)),
            jnp.where(lane_of == 0, west, pltpu.roll(x, 1, axis=1)),
        )

    def edge_copy(stage, d):
        return pltpu.make_async_remote_copy(
            src_ref=edge_send.at[stage, d],
            dst_ref=edge_recv.at[stage, OPPOSITE[d]],
            send_sem=edge_ssem.at[d],
            recv_sem=edge_rsem.at[SENT_AT[stage, d]],
            device_id=where_to[d],
            device_id_type=MESH,
        )

    def edge_arrival(stage, d):
        at = SENT_AT[stage, OPPOSITE[d]]
        return pltpu.make_async_remote_copy(
            src_ref=edge_send.at[stage, d],
            dst_ref=edge_recv.at[stage, d],
            send_sem=edge_ssem.at[OPPOSITE[d]],
            recv_sem=edge_rsem.at[at],
            device_id=where_to[d],
            device_id_type=MESH,
        )

    def drain_sums():
        sent = sum_recv.at[:, pl.ds(0, n - 1)]
        pltpu.make_async_copy(sent, sent, sum_ssem).wait()

    def drain_edges():
        for d in EVERY:
            sent = edge_send.at[0, pl.ds(0, sum(d in ways for ways in SENT))]
            pl.when(has[d])(pltpu.make_async_copy(sent, sent, edge_ssem.at[d]).wait)

    def diag_copy(i):
        return pltpu.make_async_remote_copy(
            src_ref=diag_send.at[i],
            dst_ref=diag_recv.at[i],
            send_sem=diag_ssem.at[i],
            recv_sem=diag_rsem.at[i],
            device_id=diag_to[i],
            device_id_type=MESH,
        )

    def send_edges(stage, ways):
        for d in ways:
            pl.when(has[d])(edge_copy(stage, d).start)

    def wait_edges(stage, sides):
        for d in sides:
            pl.when(has[d])(edge_arrival(stage, d).wait_recv)

    def edge_rows(d, x):
        if d < 2:
            at = rows - 1 if d == NORTH else 0
            return [part[at : at + 1] for part in x]
        at = lanes - 1 if d == EAST else 0
        return [col_to_row([part[:, at : at + 1] for part in x])]

    def put_edge(stage, d, x, slot):
        for i, row in enumerate(edge_rows(d, x)):
            edge_send[stage, d, slot + i : slot + i + 1] = row

    def keep_sums(phase, row):
        sum_send[phase] = row
        sum_recv[phase, me] = row

    def send_sums(phase):
        to_all(
            lambda device: pltpu.make_async_remote_copy(
                src_ref=sum_send.at[phase],
                dst_ref=sum_recv.at[phase, me],
                send_sem=sum_ssem,
                recv_sem=sum_rsem.at[phase],
                device_id=device,
                device_id_type=MESH,
            ).start()
        )

    def wait_sums(phase):
        others = sum_recv.at[phase, pl.ds(0, n - 1)]
        pltpu.make_async_copy(others, others, sum_rsem.at[phase]).wait()
        if n > 64:
            return jnp.sum(sum_recv[phase], axis=0)
        parts = [sum_recv[phase, i] for i in range(n)]
        while len(parts) > 1:
            odd = parts[len(parts) // 2 * 2 :]
            parts = [a + b for a, b in zip(parts[::2], parts[1::2])] + odd
        return parts[0]

    def spread(row, at):
        return jnp.broadcast_to(row[:, at : at + 1], (1, lanes))

    def total_row(blocks, sums):
        if sums:
            pad = jnp.zeros((rows - len(sums), lanes), F32)
            blocks = blocks + [jnp.concatenate(sums + [pad], axis=0)]
        out = None
        for i, block in enumerate(blocks):
            col = jnp.sum(block, axis=1, keepdims=True)
            term = jnp.where(lane_of == row_of + i * rows, col, 0.0)
            out = term if out is None else out + term
        return jnp.sum(out, axis=0, keepdims=True)

    def project(x):
        acc = None
        for c in range(comps):
            for r in range(rows):
                term = basis_t[c, r] * x[c][r : r + 1]
                acc = term if acc is None else acc + term
        return [acc[i : i + rows] for i in range(0, basis, rows)]

    def lift(block, coeffs):
        return jnp.sum(block * coeffs, axis=0, keepdims=True)

    def lift_all(coeffs):
        return [
            jnp.concatenate([lift(basis_t[c, r], coeffs) for r in range(rows)], axis=0)
            for c in range(comps)
        ]

    def inner(xs, ys):
        out = None
        for x, y in zip(xs, ys):
            term = jnp.sum(x * y, axis=0, keepdims=True)
            out = term if out is None else out + term
        return out

    for load in small:
        load.wait()
    gram_full[my_col] = gram_ref[...]
    right = [r_ref[c] for c in range(comps)]
    free = [mask_ref[c].astype(F32) for c in range(comps)]
    visc = visc_ref[...]
    for d in EVERY:
        put_edge(0, d, [visc], 2 * comps if d < 2 else 2)
    for d in (NORTH, EAST):
        put_edge(0, d, right, 0)
        put_edge(0, d, free, comps if d < 2 else 1)

    row_copy = pltpu.make_async_remote_copy(
        src_ref=basis_t.at[:, rows - 1],
        dst_ref=row_recv,
        send_sem=row_ssem,
        recv_sem=row_rsem,
        device_id=where_to[NORTH],
        device_id_type=MESH,
    )
    col_copy = pltpu.make_async_remote_copy(
        src_ref=col_send,
        dst_ref=col_recv,
        send_sem=col_ssem,
        recv_sem=col_rsem,
        device_id=where_to[EAST],
        device_id_type=MESH,
    )

    def gram_copy(i):
        return pltpu.make_async_remote_copy(
            src_ref=gram_ref,
            dst_ref=gram_full.at[my_col],
            send_sem=gram_ssem,
            recv_sem=gram_rsem,
            device_id=(my_row, lax.rem(my_col + i, ncol)),
            device_id_type=MESH,
        )

    pl.semaphore_wait(barrier, greeted)
    tell_lower()
    send_edges(0, EVERY)
    pltpu.make_async_copy(basis_t, basis_t, load_sem).wait()
    pl.when(has[NORTH])(row_copy.start)
    keep_sums(0, total_row(project(right), []))

    pl.when(top)(lambda: send_sums(0))
    for i in range(1, ncol):
        gram_copy(i).start()

    column = jnp.zeros((basis, lanes), F32)
    for c in range(comps):
        for r in range(rows):
            spot = c * rows + r
            turned = pltpu.roll(basis_t[c, r], (spot + 1) % lanes, axis=1)
            column = jnp.where(wide_lane == spot, turned, column)
    col_send[...] = column
    pl.when(has[EAST])(col_copy.start)

    def hear_and_send():
        hear_higher()
        send_sums(0)

    pl.when(above)(hear_and_send)

    wait_edges(0, (EAST, WEST))
    sides = [row_to_cols(edge_recv[0, d, 2:3])[0] for d in (EAST, WEST)]
    _, below_visc, *beside = shifted(visc, 0.0, 0.0, *sides)
    open_north = 1.0 + 0.5 * (visc + below_visc)
    for v in beside:
        open_north = open_north + 0.5 * (visc + v)
    edge_send[1, NORTH, 0:1] = open_north[rows - 1 : rows]
    send_edges(1, (NORTH,))

    wait_edges(0, (NORTH, SOUTH))
    visc_halo = [edge_recv[0, d, 2 * comps : 2 * comps + 1] for d in (NORTH, SOUTH)]
    faces = [0.5 * (visc + v) for v in shifted(visc, *visc_halo, *sides)]
    diagonal = 1.0 + faces[0] + faces[1] + faces[2] + faces[3]
    inverse = 1.0 / diagonal
    scaled = [u * inverse for u in free]
    jacobi = [s + (1.0 - u) for s, u in zip(scaled, free)]
    put_edge(1, EAST, scaled, 0)
    send_edges(1, (EAST,))

    pl.when(has[SOUTH])(row_copy.wait_recv)
    pl.when(has[WEST])(col_copy.wait_recv)
    others = gram_full.at[pl.ds(0, ncol - 1)]
    pltpu.make_async_copy(others, others, gram_rsem).wait()
    gram = gram_full[...].reshape(basis, basis)
    wait_edges(1, (SOUTH, WEST))
    south_right = [edge_recv[0, SOUTH, c : c + 1] for c in range(comps)]
    south_free = [edge_recv[0, SOUTH, comps + c : comps + c + 1] for c in range(comps)]
    south_inverse = 1.0 / jnp.where(
        has[SOUTH], edge_recv[1, SOUTH, 0:1] + faces[1][0:1], 1.0
    )
    south_scaled = [u * south_inverse for u in south_free]
    west_right, west_free = edge_recv[0, WEST, 0:1], edge_recv[0, WEST, 1:2]
    west_scaled = edge_recv[1, WEST, 0:1]

    def halo_values(lifted, south_res, west_res):
        south = [
            a * r + u * b
            for a, r, u, b in zip(south_scaled, south_res, south_free, lifted[0])
        ]
        return south, west_scaled * west_res + west_free * lifted[1]

    def lift_halos(coeffs):
        south = [lift(row_recv[c], coeffs) for c in range(comps)]
        return south, lift(col_recv[...], coeffs)

    def operate(x, south, west):
        west_cols = row_to_cols(west)
        out, to_south, to_west = [], [], []
        for c in range(comps):
            masked = free[c] * x[c]
            around = shifted(masked, 0.0, south[c], 0.0, west_cols[c])
            stencil = diagonal * masked - (
                faces[0] * around[0]
                + faces[1] * around[1]
                + faces[2] * around[2]
                + faces[3] * around[3]
            )
            out.append(free[c] * stencil + (1.0 - free[c]) * x[c])
            to_south.append(faces[1] * masked)
            to_west.append(faces[3] * masked)
        return out, to_south, to_west

    def put_terms(stage, to_south, to_west):
        south_rows = edge_rows(SOUTH, to_south)
        west_row = edge_rows(WEST, to_west)[0]
        for c in range(comps):
            edge_send[stage, SOUTH, c : c + 1] = south_rows[c]
        edge_send[stage, WEST, 0:1] = west_row
        return [-u * q for u, q in zip(south_free, south_rows)], -west_free * west_row

    def cross(south, west, south_term, west_term):
        total = west * west_term
        for a, b in zip(south, south_term):
            total = total + a * b
        return total

    def complete(stage, image):
        east_cols = row_to_cols(edge_recv[stage, EAST, 0:1])
        return [
            image[c]
            - free[c]
            * (
                jnp.where(row_of == rows - 1, edge_recv[stage, NORTH, c : c + 1], 0.0)
                + jnp.where(lane_of == lanes - 1, east_cols[c], 0.0)
            )
            for c in range(comps)
        ]

    def solve(dot):
        return jnp.sum(gram * dot[:, :basis], axis=1, keepdims=True) * scale

    dot = wait_sums(0)
    coeffs = solve(dot)
    lifted, lifted_halos = lift_all(coeffs), lift_halos(coeffs)
    direction = [j * r + b for j, r, b in zip(jacobi, right, lifted)]
    south, west = halo_values(lifted_halos, south_right, west_right)
    image, to_south, to_west = operate(direction, south, west)
    south_term, west_term = put_terms(2, to_south, to_west)
    across = project(image)
    extra = col_recv[...] * west_term
    for c in range(comps):
        extra = extra + row_recv[c] * south_term[c]
    across = [a + extra[i * rows : (i + 1) * rows] for i, a in enumerate(across)]
    second = total_row(
        across,
        [
            inner(right, direction),
            inner(direction, image) + cross(south, west, south_term, west_term),
        ],
    )
    keep_sums(1, second)
    send_sums(1)
    for d in (NORTH, EAST):
        put_edge(2, d, image, 0)
    corner_row = jnp.where(row_of == rows - 1, 1.0, 0.0)
    turned = [pltpu.roll(q, lanes - 1, axis=1) for q in to_west]
    for c in range(comps):
        diag_send[0, c : c + 1] = jnp.where(
            lane_of == lanes - 1, turned[c], 0.0
        )[rows - 1 : rows]
    turned = [pltpu.roll(q, rows - 1, axis=0) * corner_row for q in to_south]
    diag_send[1, 0:1] = col_to_row([q[:, lanes - 1 : lanes] for q in turned])
    send_edges(2, EVERY)
    for i in range(2):
        pl.when(has_diag[i])(diag_copy(i).start)
    wait_edges(2, EVERY)
    for i in range(2):
        pl.when(has_diag[1 - i])(diag_copy(i).wait_recv)
    image = complete(2, image)
    south_image = [
        edge_recv[2, SOUTH, c : c + 1]
        + south_term[c]
        - south_free[c] * diag_recv[0, c : c + 1]
        for c in range(comps)
    ]
    west_image = edge_recv[2, WEST, 0:1] + west_term - west_free * diag_recv[1, 0:1]
    sums = wait_sums(1)
    energy, curve = spread(sums, basis), spread(sums, basis + 1)
    step = energy / curve
    coeffs = solve(sums)
    residual = [r - step * w for r, w in zip(right, image)]
    smoothed = [
        j * r + (b - step * l)
        for j, r, b, l in zip(jacobi, residual, lifted, lift_all(coeffs))
    ]
    south_lift, west_lift = lift_halos(coeffs)
    south, west = halo_values(
        (
            [b - step * l for b, l in zip(lifted_halos[0], south_lift)],
            lifted_halos[1] - step * west_lift,
        ),
        [r - step * w for r, w in zip(south_right, south_image)],
        west_right - step * west_image,
    )
    smoothed_image, to_south, to_west = operate(smoothed, south, west)
    south_term, west_term = put_terms(3, to_south, to_west)
    third = total_row(
        [],
        [
            inner(residual, smoothed),
            inner(smoothed, image),
            inner(smoothed, smoothed_image)
            + cross(south, west, south_term, west_term),
        ],
    )
    keep_sums(2, third)
    send_sums(2)
    send_edges(3, (SOUTH, WEST))
    wait_edges(3, (NORTH, EAST))
    smoothed_image = complete(3, smoothed_image)
    for i in range(2):
        pl.when(has_diag[i])(diag_copy(i).wait_send)
    pl.when(has[NORTH])(row_copy.wait_send)
    pl.when(has[EAST])(col_copy.wait_send)
    pltpu.make_async_copy(others, others, gram_ssem).wait()
    sums = wait_sums(2)
    energy_new = spread(sums, 0)
    ratio = energy_new / energy
    curve_new = spread(sums, 2) + ratio * (2.0 * spread(sums, 1) + ratio * curve)
    step_new = energy_new / curve_new
    for c in range(comps):
        out_ref[c] = step * direction[c] + step_new * (smoothed[c] + ratio * direction[c])
        out_ref[comps + c] = residual[c] - step_new * (smoothed_image[c] + ratio * image[c])

    drain_sums()
    drain_edges()


def on_device(nrow, ncol, right_side, viscosity, free_mask, coarse_basis, gram_inverse):
    comps, rows, lanes = right_side.shape
    basis = coarse_basis.shape[0]
    n = nrow * ncol
    unknowns = comps * rows * lanes * n * basis
    scale = 1.0 / (32.0 * math.sqrt(float(unknowns)))
    vmem = pl.BlockSpec(memory_space=pltpu.VMEM)
    dma = pltpu.SemaphoreType.DMA
    out = pl.pallas_call(
        functools.partial(kernel, nrow, ncol, scale),
        out_shape=pltpu.VMEM((2 * comps, rows, lanes), F32),
        in_specs=[pl.BlockSpec(memory_space=pltpu.HBM)] * 5,
        out_specs=vmem,
        scratch_shapes=[
            pltpu.VMEM(right_side.shape, F32),
            pltpu.VMEM(viscosity.shape, F32),
            pltpu.VMEM(free_mask.shape, free_mask.dtype),
            pltpu.VMEM(gram_inverse.shape, F32),
            pltpu.VMEM((comps, rows, basis, lanes), F32),
            pltpu.VMEM((comps, basis, lanes), F32),
            pltpu.VMEM((basis, lanes), F32),
            pltpu.VMEM((basis, lanes), F32),
            pltpu.VMEM((4, 4, 8, lanes), F32),
            pltpu.VMEM((4, 4, 8, lanes), F32),
            pltpu.VMEM((2, 8, lanes), F32),
            pltpu.VMEM((2, 8, lanes), F32),
            pltpu.VMEM((ncol,) + gram_inverse.shape, F32),
            pltpu.VMEM((3, 1, lanes), F32),
            pltpu.VMEM((3, n, 1, lanes), F32),
            dma,
            dma((4,)),
            dma,
            dma,
            dma,
            dma,
            dma((4,)),
            dma((len(SENT_AT),)),
            dma((2,)),
            dma((2,)),
            dma,
            dma,
            dma,
            dma((3,)),
            pltpu.SemaphoreType.REGULAR,
        ],
        compiler_params=pltpu.CompilerParams(
            collective_id=0, has_side_effects=True, vmem_limit_bytes=60_000_000
        ),
    )(right_side, viscosity, free_mask, coarse_basis, gram_inverse)
    return out[:comps], out[comps:]


def solution(mesh):
    in_specs = (
        P(None, "row", "col"),
        P("row", "col"),
        P(None, "row", "col"),
        P(None, None, "row", "col"),
        P("col", None),
    )
    out_specs = (P(None, "row", "col"), P(None, "row", "col"))
    return jax.shard_map(
        functools.partial(on_device, mesh.shape["row"], mesh.shape["col"]),
        mesh=mesh,
        in_specs=in_specs,
        out_specs=out_specs,
        check_vma=False,
    )
```

```python
import functools
import math

import jax
import jax.numpy as jnp
from jax import lax
from jax.experimental import pallas as pl
from jax.experimental.pallas import tpu as pltpu
from jax.sharding import PartitionSpec as P

MESH = pl.DeviceIdType.MESH
HIGH = lax.Precision.HIGHEST
F32 = jnp.float32
OPPOSITE = (1, 0, 3, 2)
NORTH, SOUTH, EAST, WEST = range(4)
EVERY = (NORTH, SOUTH, EAST, WEST)
SENT = (EVERY, (NORTH, EAST), EVERY, (SOUTH, WEST))
SENT_AT = {}
for _stage, _ways in enumerate(SENT):
    for _way in _ways:
        SENT_AT[_stage, _way] = len(SENT_AT)


def zigzag(n):
    order = []
    for i in range(1, n // 2 + 1):
        order += [i, n - i] if 2 * i != n else [i]
    return order


def plane_rows(nrow):
    return max(d for d in range(1, nrow + 1) if nrow % d == 0 and d * d <= nrow)


def kernel(
    nrow,
    ncol,
    scale,
    r_hbm,
    visc_hbm,
    mask_hbm,
    basis_ref,
    gram_hbm,
    out_ref,
    r_ref,
    visc_ref,
    mask_ref,
    gram_ref,
    basis_t,
    row_recv,
    col_send,
    col_recv,
    edge_send,
    edge_recv,
    diag_send,
    diag_recv,
    gram_full,
    sum_send,
    sum_recv,
    load_sem,
    small_sem,
    row_ssem,
    row_rsem,
    col_ssem,
    col_rsem,
    edge_ssem,
    edge_rsem,
    diag_ssem,
    diag_rsem,
    gram_ssem,
    gram_rsem,
    sum_ssem,
    sum_rsem,
    chain_sem,
):
    comps, rows, lanes = r_ref.shape
    basis = basis_ref.shape[0]
    cells = comps * rows
    n = nrow * ncol
    my_row, my_col = lax.axis_index("row"), lax.axis_index("col")
    me = my_row * ncol + my_col
    has = (my_row < nrow - 1, my_row > 0, my_col < ncol - 1, my_col > 0)
    where_to = (
        (my_row + 1, my_col),
        (my_row - 1, my_col),
        (my_row, my_col + 1),
        (my_row, my_col - 1),
    )

    has_diag = (
        jnp.logical_and(has[NORTH], has[WEST]),
        jnp.logical_and(has[SOUTH], has[EAST]),
    )
    diag_to = ((my_row + 1, my_col - 1), (my_row - 1, my_col + 1))

    loads = [
        pltpu.make_async_copy(
            basis_ref.at[:, c, r], basis_t.at[c, r], load_sem
        )
        for c in range(comps)
        for r in range(rows)
    ]
    small = [
        pltpu.make_async_copy(src, dst, small_sem.at[i])
        for i, (src, dst) in enumerate(
            (
                (r_hbm, r_ref),
                (visc_hbm, visc_ref),
                (mask_hbm, mask_ref),
                (gram_hbm, gram_ref),
            )
        )
    ]
    for load in small + loads:
        load.start()

    barrier = pltpu.get_barrier_semaphore()

    def target(dr, dc):
        return lax.rem(my_row + dr, nrow), lax.rem(my_col + dc, ncol)

    def to_all(act):
        if n <= 64:
            rows_to = [lax.rem(my_row + dr, nrow) for dr in range(nrow)]
            cols_to = [lax.rem(my_col + dc, ncol) for dc in range(ncol)]
            for dr in zigzag(nrow) + [0]:
                for dc in zigzag(ncol) + [0]:
                    if dr or dc:
                        act((rows_to[dr], cols_to[dc]))
            return

        def one(i, carry):
            t = lax.rem(me + i, n)
            act((t // ncol, lax.rem(t, ncol)))
            return carry

        lax.fori_loop(1, n, one, 0)

    depth = plane_rows(nrow)
    planes = nrow // depth
    group = depth * ncol
    plane, spot_row = my_row // depth, lax.rem(my_row, depth)
    mine = spot_row * ncol + my_col
    above, below = plane < planes - 1, plane > 0

    def greet(device):
        pl.semaphore_signal(barrier, inc=1, device_id=device, device_id_type=MESH)

    cross_down = jnp.logical_and(below, spot_row == 0)
    cross_up = jnp.logical_and(above, spot_row == depth - 1)
    greeted = plane * group + group - 1 + jnp.where(cross_up, 1, 0)
    pl.when(cross_down)(functools.partial(greet, (my_row - 1, my_col)))

    for dr in zigzag(depth) + [0]:
        row = plane * depth + lax.rem(spot_row + dr, depth)
        for dc in zigzag(ncol) + [0]:
            if dr or dc:
                greet((row, lax.rem(my_col + dc, ncol)))
    def greet_higher(i, carry):
        t = (plane + 1) * group + i
        greet((t // ncol, lax.rem(t, ncol)))
        return carry

    lax.fori_loop(0, (planes - 1 - plane) * group, greet_higher, 0)

    def tell_lower():
        def tell(q, carry):
            pl.semaphore_signal(
                chain_sem,
                inc=1,
                device_id=(q * depth + spot_row, my_col),
                device_id_type=MESH,
            )
            return carry

        lax.fori_loop(0, plane, tell, 0)

    def hear_higher():
        pl.when(above)(lambda: pl.semaphore_wait(chain_sem, planes - 1 - plane))

    top = jnp.logical_not(above)

    for d in range(4):

        @pl.when(jnp.logical_not(has[d]))
        def _(d=d):
            for stage in range(4):
                edge_recv[stage, d] = jnp.zeros(edge_recv.shape[2:], F32)
            if d == SOUTH:
                row_recv[...] = jnp.zeros(row_recv.shape, F32)
            if d == WEST:
                col_recv[...] = jnp.zeros(col_recv.shape, F32)

    for i in range(2):

        @pl.when(jnp.logical_not(has_diag[1 - i]))
        def _(i=i):
            diag_recv[i] = jnp.zeros(diag_recv.shape[1:], F32)

    lane_of = lax.broadcasted_iota(jnp.int32, (rows, lanes), 1)
    row_of = lax.broadcasted_iota(jnp.int32, (rows, lanes), 0)
    diag_mask = [lane_of == row_of + c * rows for c in range(comps)]
    wide_lane = lax.broadcasted_iota(jnp.int32, (basis, lanes), 1)

    def col_to_row(cols):
        out = None
        for c, col in enumerate(cols):
            term = jnp.sum(
                jnp.where(diag_mask[c], jnp.broadcast_to(col, (rows, lanes)), 0.0),
                axis=0,
                keepdims=True,
            )
            out = term if out is None else out + term
        return out

    def row_to_cols(row):
        wide = jnp.broadcast_to(row, (rows, lanes))
        return [
            jnp.sum(jnp.where(diag_mask[c], wide, 0.0), axis=1, keepdims=True)
            for c in range(comps)
        ]

    def shifted(x, north, south, east, west):
        return (
            jnp.where(row_of == rows - 1, north, pltpu.roll(x, rows - 1, axis=0)),
            jnp.where(row_of == 0, south, pltpu.roll(x, 1, axis=0)),
            jnp.where(lane_of == lanes - 1, east, pltpu.roll(x, lanes - 1, axis=1)),
            jnp.where(lane_of == 0, west, pltpu.roll(x, 1, axis=1)),
        )

    def edge_copy(stage, d):
        return pltpu.make_async_remote_copy(
            src_ref=edge_send.at[stage, d],
            dst_ref=edge_recv.at[stage, OPPOSITE[d]],
            send_sem=edge_ssem.at[d],
            recv_sem=edge_rsem.at[SENT_AT[stage, d]],
            device_id=where_to[d],
            device_id_type=MESH,
        )

    def edge_arrival(stage, d):
        at = SENT_AT[stage, OPPOSITE[d]]
        return pltpu.make_async_remote_copy(
            src_ref=edge_send.at[stage, d],
            dst_ref=edge_recv.at[stage, d],
            send_sem=edge_ssem.at[OPPOSITE[d]],
            recv_sem=edge_rsem.at[at],
            device_id=where_to[d],
            device_id_type=MESH,
        )

    def drain_sums():
        sent = sum_recv.at[:, pl.ds(0, n - 1)]
        pltpu.make_async_copy(sent, sent, sum_ssem).wait()

    def drain_edges():
        for d in EVERY:
            sent = edge_send.at[0, pl.ds(0, sum(d in ways for ways in SENT))]
            pl.when(has[d])(pltpu.make_async_copy(sent, sent, edge_ssem.at[d]).wait)

    def diag_copy(i):
        return pltpu.make_async_remote_copy(
            src_ref=diag_send.at[i],
            dst_ref=diag_recv.at[i],
            send_sem=diag_ssem.at[i],
            recv_sem=diag_rsem.at[i],
            device_id=diag_to[i],
            device_id_type=MESH,
        )

    def send_edges(stage, ways):
        for d in ways:
            pl.when(has[d])(edge_copy(stage, d).start)

    def wait_edges(stage, sides):
        for d in sides:
            pl.when(has[d])(edge_arrival(stage, d).wait_recv)

    def edge_rows(d, x):
        if d < 2:
            at = rows - 1 if d == NORTH else 0
            return [part[at : at + 1] for part in x]
        at = lanes - 1 if d == EAST else 0
        return [col_to_row([part[:, at : at + 1] for part in x])]

    def put_edge(stage, d, x, slot):
        for i, row in enumerate(edge_rows(d, x)):
            edge_send[stage, d, slot + i : slot + i + 1] = row

    def keep_sums(phase, row):
        sum_send[phase] = row
        sum_recv[phase, me] = row

    def send_sums(phase):
        to_all(
            lambda device: pltpu.make_async_remote_copy(
                src_ref=sum_send.at[phase],
                dst_ref=sum_recv.at[phase, me],
                send_sem=sum_ssem,
                recv_sem=sum_rsem.at[phase],
                device_id=device,
                device_id_type=MESH,
            ).start()
        )

    def wait_sums(phase):
        others = sum_recv.at[phase, pl.ds(0, n - 1)]
        pltpu.make_async_copy(others, others, sum_rsem.at[phase]).wait()
        if n > 64:
            return jnp.sum(sum_recv[phase], axis=0)
        parts = [sum_recv[phase, i] for i in range(n)]
        while len(parts) > 1:
            odd = parts[len(parts) // 2 * 2 :]
            parts = [a + b for a, b in zip(parts[::2], parts[1::2])] + odd
        return parts[0]

    def spread(row, at):
        return jnp.broadcast_to(row[:, at : at + 1], (1, lanes))

    def total_row(blocks, tiles):
        out = None
        for i, block in enumerate(blocks):
            col = jnp.sum(block, axis=1, keepdims=True)
            term = jnp.where(lane_of == row_of + i * rows, col, 0.0)
            out = term if out is None else out + term
        for i, tile in enumerate(tiles):
            col = jnp.sum(tile, axis=1, keepdims=True)
            term = jnp.where(lane_of == len(blocks) * rows + i, col, 0.0)
            out = term if out is None else out + term
        return jnp.sum(out, axis=0, keepdims=True)

    def project(x):
        acc = None
        for c in range(comps):
            for r in range(rows):
                term = basis_t[c, r] * x[c][r : r + 1]
                acc = term if acc is None else acc + term
        return [acc[i : i + rows] for i in range(0, basis, rows)]

    def lift(block, coeffs):
        return jnp.sum(block * coeffs, axis=0, keepdims=True)

    def lift_all(coeffs):
        return [
            jnp.concatenate([lift(basis_t[c, r], coeffs) for r in range(rows)], axis=0)
            for c in range(comps)
        ]

    def inner(xs, ys):
        out = None
        for x, y in zip(xs, ys):
            out = x * y if out is None else out + x * y
        return out

    for load in small:
        load.wait()
    gram_full[my_col] = gram_ref[...]
    right = [r_ref[c] for c in range(comps)]
    free = [mask_ref[c].astype(F32) for c in range(comps)]
    visc = visc_ref[...]
    for d in EVERY:
        put_edge(0, d, [visc], 2 * comps if d < 2 else 2)
    for d in (NORTH, EAST):
        put_edge(0, d, right, 0)
        put_edge(0, d, free, comps if d < 2 else 1)

    row_copy = pltpu.make_async_remote_copy(
        src_ref=basis_t.at[:, rows - 1],
        dst_ref=row_recv,
        send_sem=row_ssem,
        recv_sem=row_rsem,
        device_id=where_to[NORTH],
        device_id_type=MESH,
    )
    col_copy = pltpu.make_async_remote_copy(
        src_ref=col_send,
        dst_ref=col_recv,
        send_sem=col_ssem,
        recv_sem=col_rsem,
        device_id=where_to[EAST],
        device_id_type=MESH,
    )

    def gram_copy(i):
        return pltpu.make_async_remote_copy(
            src_ref=gram_ref,
            dst_ref=gram_full.at[my_col],
            send_sem=gram_ssem,
            recv_sem=gram_rsem,
            device_id=(my_row, lax.rem(my_col + i, ncol)),
            device_id_type=MESH,
        )

    pl.semaphore_wait(barrier, greeted)
    tell_lower()
    send_edges(0, EVERY)
    pltpu.make_async_copy(basis_t, basis_t, load_sem).wait()
    keep_sums(0, total_row(project(right), []))

    pl.when(top)(lambda: send_sums(0))
    pl.when(has[NORTH])(row_copy.start)
    for i in range(1, ncol):
        gram_copy(i).start()

    column = jnp.zeros((basis, lanes), F32)
    for c in range(comps):
        for r in range(rows):
            spot = c * rows + r
            turned = pltpu.roll(basis_t[c, r], (spot + 1) % lanes, axis=1)
            column = jnp.where(wide_lane == spot, turned, column)
    col_send[...] = column
    pl.when(has[EAST])(col_copy.start)

    def hear_and_send():
        hear_higher()
        send_sums(0)

    pl.when(above)(hear_and_send)

    wait_edges(0, (EAST, WEST))
    sides = [row_to_cols(edge_recv[0, d, 2:3])[0] for d in (EAST, WEST)]
    _, below_visc, *beside = shifted(visc, 0.0, 0.0, *sides)
    open_north = 1.0 + 0.5 * (visc + below_visc)
    for v in beside:
        open_north = open_north + 0.5 * (visc + v)
    edge_send[1, NORTH, 0:1] = open_north[rows - 1 : rows]
    send_edges(1, (NORTH,))

    wait_edges(0, (NORTH, SOUTH))
    visc_halo = [edge_recv[0, d, 2 * comps : 2 * comps + 1] for d in (NORTH, SOUTH)]
    faces = [0.5 * (visc + v) for v in shifted(visc, *visc_halo, *sides)]
    diagonal = 1.0 + faces[0] + faces[1] + faces[2] + faces[3]
    inverse = 1.0 / diagonal
    scaled = [u * inverse for u in free]
    jacobi = [s + (1.0 - u) for s, u in zip(scaled, free)]
    put_edge(1, EAST, scaled, 0)
    send_edges(1, (EAST,))

    pl.when(has[SOUTH])(row_copy.wait_recv)
    pl.when(has[WEST])(col_copy.wait_recv)
    others = gram_full.at[pl.ds(0, ncol - 1)]
    pltpu.make_async_copy(others, others, gram_rsem).wait()
    gram = gram_full[...].reshape(basis, basis)
    wait_edges(1, (SOUTH, WEST))
    south_right = [edge_recv[0, SOUTH, c : c + 1] for c in range(comps)]
    south_free = [edge_recv[0, SOUTH, comps + c : comps + c + 1] for c in range(comps)]
    south_inverse = 1.0 / jnp.where(
        has[SOUTH], edge_recv[1, SOUTH, 0:1] + faces[1][0:1], 1.0
    )
    south_scaled = [u * south_inverse for u in south_free]
    west_right, west_free = edge_recv[0, WEST, 0:1], edge_recv[0, WEST, 1:2]
    west_scaled = edge_recv[1, WEST, 0:1]

    def halo_values(lifted, south_res, west_res):
        south = [
            a * r + u * b
            for a, r, u, b in zip(south_scaled, south_res, south_free, lifted[0])
        ]
        return south, west_scaled * west_res + west_free * lifted[1]

    def lift_halos(coeffs):
        south = [lift(row_recv[c], coeffs) for c in range(comps)]
        return south, lift(col_recv[...], coeffs)

    def operate(x, south, west):
        west_cols = row_to_cols(west)
        out, to_south, to_west = [], [], []
        for c in range(comps):
            masked = free[c] * x[c]
            around = shifted(masked, 0.0, south[c], 0.0, west_cols[c])
            stencil = diagonal * masked - (
                faces[0] * around[0]
                + faces[1] * around[1]
                + faces[2] * around[2]
                + faces[3] * around[3]
            )
            out.append(free[c] * stencil + (1.0 - free[c]) * x[c])
            to_south.append(faces[1] * masked)
            to_west.append(faces[3] * masked)
        return out, to_south, to_west

    def put_terms(stage, to_south, to_west):
        south_rows = edge_rows(SOUTH, to_south)
        west_row = edge_rows(WEST, to_west)[0]
        for c in range(comps):
            edge_send[stage, SOUTH, c : c + 1] = south_rows[c]
        edge_send[stage, WEST, 0:1] = west_row
        return [-u * q for u, q in zip(south_free, south_rows)], -west_free * west_row

    def cross(south, west, south_term, west_term):
        total = west * west_term
        for a, b in zip(south, south_term):
            total = total + a * b
        return jnp.where(row_of == 0, total, 0.0)

    def complete(stage, image):
        east_cols = row_to_cols(edge_recv[stage, EAST, 0:1])
        return [
            image[c]
            - free[c]
            * (
                jnp.where(row_of == rows - 1, edge_recv[stage, NORTH, c : c + 1], 0.0)
                + jnp.where(lane_of == lanes - 1, east_cols[c], 0.0)
            )
            for c in range(comps)
        ]

    def solve(dot):
        return jnp.sum(gram * dot[:, :basis], axis=1, keepdims=True) * scale

    dot = wait_sums(0)
    coeffs = solve(dot)
    lifted, lifted_halos = lift_all(coeffs), lift_halos(coeffs)
    direction = [j * r + b for j, r, b in zip(jacobi, right, lifted)]
    south, west = halo_values(lifted_halos, south_right, west_right)
    image, to_south, to_west = operate(direction, south, west)
    south_term, west_term = put_terms(2, to_south, to_west)
    across = project(image)
    extra = col_recv[...] * west_term
    for c in range(comps):
        extra = extra + row_recv[c] * south_term[c]
    across = [a + extra[i * rows : (i + 1) * rows] for i, a in enumerate(across)]
    second = total_row(
        across,
        [
            inner(right, direction),
            inner(direction, image) + cross(south, west, south_term, west_term),
        ],
    )
    keep_sums(1, second)
    send_sums(1)
    for d in (NORTH, EAST):
        put_edge(2, d, image, 0)
    corner_row = jnp.where(row_of == rows - 1, 1.0, 0.0)
    turned = [pltpu.roll(q, lanes - 1, axis=1) for q in to_west]
    for c in range(comps):
        diag_send[0, c : c + 1] = jnp.where(
            lane_of == lanes - 1, turned[c], 0.0
        )[rows - 1 : rows]
    turned = [pltpu.roll(q, rows - 1, axis=0) * corner_row for q in to_south]
    diag_send[1, 0:1] = col_to_row([q[:, lanes - 1 : lanes] for q in turned])
    send_edges(2, EVERY)
    for i in range(2):
        pl.when(has_diag[i])(diag_copy(i).start)
    wait_edges(2, EVERY)
    for i in range(2):
        pl.when(has_diag[1 - i])(diag_copy(i).wait_recv)
    image = complete(2, image)
    south_image = [
        edge_recv[2, SOUTH, c : c + 1]
        + south_term[c]
        - south_free[c] * diag_recv[0, c : c + 1]
        for c in range(comps)
    ]
    west_image = edge_recv[2, WEST, 0:1] + west_term - west_free * diag_recv[1, 0:1]
    sums = wait_sums(1)
    energy, curve = spread(sums, basis), spread(sums, basis + 1)
    step = energy / curve
    coeffs = solve(sums)
    residual = [r - step * w for r, w in zip(right, image)]
    smoothed = [
        j * r + (b - step * l)
        for j, r, b, l in zip(jacobi, residual, lifted, lift_all(coeffs))
    ]
    south_lift, west_lift = lift_halos(coeffs)
    south, west = halo_values(
        (
            [b - step * l for b, l in zip(lifted_halos[0], south_lift)],
            lifted_halos[1] - step * west_lift,
        ),
        [r - step * w for r, w in zip(south_right, south_image)],
        west_right - step * west_image,
    )
    smoothed_image, to_south, to_west = operate(smoothed, south, west)
    south_term, west_term = put_terms(3, to_south, to_west)
    third = total_row(
        [],
        [
            inner(residual, smoothed),
            inner(smoothed, image),
            inner(smoothed, smoothed_image)
            + cross(south, west, south_term, west_term),
        ],
    )
    keep_sums(2, third)
    send_sums(2)
    send_edges(3, (SOUTH, WEST))
    wait_edges(3, (NORTH, EAST))
    smoothed_image = complete(3, smoothed_image)
    for i in range(2):
        pl.when(has_diag[i])(diag_copy(i).wait_send)
    pl.when(has[NORTH])(row_copy.wait_send)
    pl.when(has[EAST])(col_copy.wait_send)
    pltpu.make_async_copy(others, others, gram_ssem).wait()
    sums = wait_sums(2)
    energy_new = spread(sums, 0)
    ratio = energy_new / energy
    curve_new = spread(sums, 2) + ratio * (2.0 * spread(sums, 1) + ratio * curve)
    step_new = energy_new / curve_new
    for c in range(comps):
        out_ref[c] = step * direction[c] + step_new * (smoothed[c] + ratio * direction[c])
        out_ref[comps + c] = residual[c] - step_new * (smoothed_image[c] + ratio * image[c])

    drain_sums()
    drain_edges()


def on_device(nrow, ncol, right_side, viscosity, free_mask, coarse_basis, gram_inverse):
    comps, rows, lanes = right_side.shape
    basis = coarse_basis.shape[0]
    n = nrow * ncol
    unknowns = comps * rows * lanes * n * basis
    scale = 1.0 / (32.0 * math.sqrt(float(unknowns)))
    vmem = pl.BlockSpec(memory_space=pltpu.VMEM)
    dma = pltpu.SemaphoreType.DMA
    out = pl.pallas_call(
        functools.partial(kernel, nrow, ncol, scale),
        out_shape=pltpu.VMEM((2 * comps, rows, lanes), F32),
        in_specs=[pl.BlockSpec(memory_space=pltpu.HBM)] * 5,
        out_specs=vmem,
        scratch_shapes=[
            pltpu.VMEM(right_side.shape, F32),
            pltpu.VMEM(viscosity.shape, F32),
            pltpu.VMEM(free_mask.shape, free_mask.dtype),
            pltpu.VMEM(gram_inverse.shape, F32),
            pltpu.VMEM((comps, rows, basis, lanes), F32),
            pltpu.VMEM((comps, basis, lanes), F32),
            pltpu.VMEM((basis, lanes), F32),
            pltpu.VMEM((basis, lanes), F32),
            pltpu.VMEM((4, 4, 8, lanes), F32),
            pltpu.VMEM((4, 4, 8, lanes), F32),
            pltpu.VMEM((2, 8, lanes), F32),
            pltpu.VMEM((2, 8, lanes), F32),
            pltpu.VMEM((ncol,) + gram_inverse.shape, F32),
            pltpu.VMEM((3, 1, lanes), F32),
            pltpu.VMEM((3, n, 1, lanes), F32),
            dma,
            dma((4,)),
            dma,
            dma,
            dma,
            dma,
            dma((4,)),
            dma((len(SENT_AT),)),
            dma((2,)),
            dma((2,)),
            dma,
            dma,
            dma,
            dma((3,)),
            pltpu.SemaphoreType.REGULAR,
        ],
        compiler_params=pltpu.CompilerParams(
            collective_id=0, has_side_effects=True, vmem_limit_bytes=60_000_000
        ),
    )(right_side, viscosity, free_mask, coarse_basis, gram_inverse)
    return out[:comps], out[comps:]


def solution(mesh):
    in_specs = (
        P(None, "row", "col"),
        P("row", "col"),
        P(None, "row", "col"),
        P(None, None, "row", "col"),
        P("col", None),
    )
    out_specs = (P(None, "row", "col"), P(None, "row", "col"))
    return jax.shard_map(
        functools.partial(on_device, mesh.shape["row"], mesh.shape["col"]),
        mesh=mesh,
        in_specs=in_specs,
        out_specs=out_specs,
        check_vma=False,
    )
```

```python
import functools
import math

import jax
import jax.numpy as jnp
from jax import lax
from jax.experimental import pallas as pl
from jax.experimental.pallas import tpu as pltpu
from jax.sharding import PartitionSpec as P

MESH = pl.DeviceIdType.MESH
HIGH = lax.Precision.HIGHEST
F32 = jnp.float32
OPPOSITE = (1, 0, 3, 2)
NORTH, SOUTH, EAST, WEST = range(4)
EVERY = (NORTH, SOUTH, EAST, WEST)
SENT = (EVERY, (NORTH, EAST), EVERY, (SOUTH, WEST))
SENT_AT = {}
for _stage, _ways in enumerate(SENT):
    for _way in _ways:
        SENT_AT[_stage, _way] = len(SENT_AT)


def zigzag(n):
    order = []
    for i in range(1, n // 2 + 1):
        order += [i, n - i] if 2 * i != n else [i]
    return order


def plane_rows(nrow):
    return max(d for d in range(1, nrow + 1) if nrow % d == 0 and d * d <= nrow)


def kernel(
    nrow,
    ncol,
    scale,
    r_hbm,
    visc_hbm,
    mask_hbm,
    basis_ref,
    gram_hbm,
    out_ref,
    r_ref,
    visc_ref,
    mask_ref,
    gram_ref,
    basis_t,
    row_recv,
    col_send,
    col_recv,
    edge_send,
    edge_recv,
    diag_send,
    diag_recv,
    gram_full,
    sum_send,
    sum_recv,
    load_sem,
    small_sem,
    row_ssem,
    row_rsem,
    col_ssem,
    col_rsem,
    edge_ssem,
    edge_rsem,
    diag_ssem,
    diag_rsem,
    gram_ssem,
    gram_rsem,
    sum_ssem,
    sum_rsem,
    chain_sem,
):
    comps, rows, lanes = r_ref.shape
    basis = basis_ref.shape[0]
    cells = comps * rows
    n = nrow * ncol
    my_row, my_col = lax.axis_index("row"), lax.axis_index("col")
    me = my_row * ncol + my_col
    has = (my_row < nrow - 1, my_row > 0, my_col < ncol - 1, my_col > 0)
    where_to = (
        (my_row + 1, my_col),
        (my_row - 1, my_col),
        (my_row, my_col + 1),
        (my_row, my_col - 1),
    )

    has_diag = (
        jnp.logical_and(has[NORTH], has[WEST]),
        jnp.logical_and(has[SOUTH], has[EAST]),
    )
    diag_to = ((my_row + 1, my_col - 1), (my_row - 1, my_col + 1))

    loads = [
        pltpu.make_async_copy(
            basis_ref.at[:, c, r], basis_t.at[c, r], load_sem
        )
        for c in range(comps)
        for r in range(rows)
    ]
    small = [
        pltpu.make_async_copy(src, dst, small_sem.at[i])
        for i, (src, dst) in enumerate(
            (
                (r_hbm, r_ref),
                (visc_hbm, visc_ref),
                (mask_hbm, mask_ref),
                (gram_hbm, gram_ref),
            )
        )
    ]
    for load in small + loads:
        load.start()

    barrier = pltpu.get_barrier_semaphore()

    def target(dr, dc):
        return lax.rem(my_row + dr, nrow), lax.rem(my_col + dc, ncol)

    def to_all(act):
        if n <= 64:
            rows_to = [lax.rem(my_row + dr, nrow) for dr in range(nrow)]
            cols_to = [lax.rem(my_col + dc, ncol) for dc in range(ncol)]
            for dr in zigzag(nrow) + [0]:
                for dc in zigzag(ncol) + [0]:
                    if dr or dc:
                        act((rows_to[dr], cols_to[dc]))
            return

        def one(i, carry):
            t = lax.rem(me + i, n)
            act((t // ncol, lax.rem(t, ncol)))
            return carry

        lax.fori_loop(1, n, one, 0)

    depth = plane_rows(nrow)
    planes = nrow // depth
    group = depth * ncol
    plane, spot_row = my_row // depth, lax.rem(my_row, depth)
    mine = spot_row * ncol + my_col
    above, below = plane < planes - 1, plane > 0

    def greet(device):
        pl.semaphore_signal(barrier, inc=1, device_id=device, device_id_type=MESH)

    cross_down = jnp.logical_and(below, spot_row == 0)
    cross_up = jnp.logical_and(above, spot_row == depth - 1)
    greeted = plane * group + group - 1 + jnp.where(cross_up, 1, 0)
    pl.when(cross_down)(functools.partial(greet, (my_row - 1, my_col)))

    for dr in zigzag(depth) + [0]:
        row = plane * depth + lax.rem(spot_row + dr, depth)
        for dc in zigzag(ncol) + [0]:
            if dr or dc:
                greet((row, lax.rem(my_col + dc, ncol)))
    def greet_higher(i, carry):
        t = (plane + 1) * group + i
        greet((t // ncol, lax.rem(t, ncol)))
        return carry

    lax.fori_loop(0, (planes - 1 - plane) * group, greet_higher, 0)

    def tell_lower():
        def tell(q, carry):
            pl.semaphore_signal(
                chain_sem.at[plane],
                inc=1,
                device_id=(q * depth + spot_row, my_col),
                device_id_type=MESH,
            )
            return carry

        lax.fori_loop(0, plane, tell, 0)

    top = jnp.logical_not(above)

    for d in range(4):

        @pl.when(jnp.logical_not(has[d]))
        def _(d=d):
            for stage in range(4):
                edge_recv[stage, d] = jnp.zeros(edge_recv.shape[2:], F32)
            if d == SOUTH:
                row_recv[...] = jnp.zeros(row_recv.shape, F32)
            if d == WEST:
                col_recv[...] = jnp.zeros(col_recv.shape, F32)

    for i in range(2):

        @pl.when(jnp.logical_not(has_diag[1 - i]))
        def _(i=i):
            diag_recv[i] = jnp.zeros(diag_recv.shape[1:], F32)

    lane_of = lax.broadcasted_iota(jnp.int32, (rows, lanes), 1)
    row_of = lax.broadcasted_iota(jnp.int32, (rows, lanes), 0)
    diag_mask = [lane_of == row_of + c * rows for c in range(comps)]
    wide_lane = lax.broadcasted_iota(jnp.int32, (basis, lanes), 1)

    def col_to_row(cols):
        out = None
        for c, col in enumerate(cols):
            term = jnp.sum(
                jnp.where(diag_mask[c], jnp.broadcast_to(col, (rows, lanes)), 0.0),
                axis=0,
                keepdims=True,
            )
            out = term if out is None else out + term
        return out

    def row_to_cols(row):
        wide = jnp.broadcast_to(row, (rows, lanes))
        return [
            jnp.sum(jnp.where(diag_mask[c], wide, 0.0), axis=1, keepdims=True)
            for c in range(comps)
        ]

    def shifted(x, north, south, east, west):
        return (
            jnp.where(row_of == rows - 1, north, pltpu.roll(x, rows - 1, axis=0)),
            jnp.where(row_of == 0, south, pltpu.roll(x, 1, axis=0)),
            jnp.where(lane_of == lanes - 1, east, pltpu.roll(x, lanes - 1, axis=1)),
            jnp.where(lane_of == 0, west, pltpu.roll(x, 1, axis=1)),
        )

    def edge_copy(stage, d):
        return pltpu.make_async_remote_copy(
            src_ref=edge_send.at[stage, d],
            dst_ref=edge_recv.at[stage, OPPOSITE[d]],
            send_sem=edge_ssem.at[d],
            recv_sem=edge_rsem.at[SENT_AT[stage, d]],
            device_id=where_to[d],
            device_id_type=MESH,
        )

    def edge_arrival(stage, d):
        at = SENT_AT[stage, OPPOSITE[d]]
        return pltpu.make_async_remote_copy(
            src_ref=edge_send.at[stage, d],
            dst_ref=edge_recv.at[stage, d],
            send_sem=edge_ssem.at[OPPOSITE[d]],
            recv_sem=edge_rsem.at[at],
            device_id=where_to[d],
            device_id_type=MESH,
        )

    def drain_sums():
        sent = sum_recv.at[:, pl.ds(0, n - 1)]
        pltpu.make_async_copy(sent, sent, sum_ssem).wait()

    def drain_edges():
        for d in EVERY:
            sent = edge_send.at[0, pl.ds(0, sum(d in ways for ways in SENT))]
            pl.when(has[d])(pltpu.make_async_copy(sent, sent, edge_ssem.at[d]).wait)

    def diag_copy(i):
        return pltpu.make_async_remote_copy(
            src_ref=diag_send.at[i],
            dst_ref=diag_recv.at[i],
            send_sem=diag_ssem.at[i],
            recv_sem=diag_rsem.at[i],
            device_id=diag_to[i],
            device_id_type=MESH,
        )

    def send_edges(stage, ways):
        for d in ways:
            pl.when(has[d])(edge_copy(stage, d).start)

    def wait_edges(stage, sides):
        for d in sides:
            pl.when(has[d])(edge_arrival(stage, d).wait_recv)

    def edge_rows(d, x):
        if d < 2:
            at = rows - 1 if d == NORTH else 0
            return [part[at : at + 1] for part in x]
        at = lanes - 1 if d == EAST else 0
        return [col_to_row([part[:, at : at + 1] for part in x])]

    def put_edge(stage, d, x, slot):
        for i, row in enumerate(edge_rows(d, x)):
            edge_send[stage, d, slot + i : slot + i + 1] = row

    def keep_sums(phase, row):
        sum_send[phase] = row
        sum_recv[phase, me] = row

    def send_to(phase, device):
        pltpu.make_async_remote_copy(
            src_ref=sum_send.at[phase],
            dst_ref=sum_recv.at[phase, me],
            send_sem=sum_ssem,
            recv_sem=sum_rsem.at[phase],
            device_id=device,
            device_id_type=MESH,
        ).start()

    def send_sums(phase):
        to_all(functools.partial(send_to, phase))

    def wait_sums(phase):
        others = sum_recv.at[phase, pl.ds(0, n - 1)]
        pltpu.make_async_copy(others, others, sum_rsem.at[phase]).wait()
        if n > 64:
            return jnp.sum(sum_recv[phase], axis=0)
        parts = [sum_recv[phase, i] for i in range(n)]
        while len(parts) > 1:
            odd = parts[len(parts) // 2 * 2 :]
            parts = [a + b for a, b in zip(parts[::2], parts[1::2])] + odd
        return parts[0]

    def spread(row, at):
        return jnp.broadcast_to(row[:, at : at + 1], (1, lanes))

    def total_row(blocks, tiles):
        out = None
        for i, block in enumerate(blocks):
            col = jnp.sum(block, axis=1, keepdims=True)
            term = jnp.where(lane_of == row_of + i * rows, col, 0.0)
            out = term if out is None else out + term
        for i, tile in enumerate(tiles):
            col = jnp.sum(tile, axis=1, keepdims=True)
            term = jnp.where(lane_of == len(blocks) * rows + i, col, 0.0)
            out = term if out is None else out + term
        return jnp.sum(out, axis=0, keepdims=True)

    def project(x):
        acc = None
        for c in range(comps):
            for r in range(rows):
                term = basis_t[c, r] * x[c][r : r + 1]
                acc = term if acc is None else acc + term
        return [acc[i : i + rows] for i in range(0, basis, rows)]

    def lift(block, coeffs):
        return jnp.sum(block * coeffs, axis=0, keepdims=True)

    def lift_all(coeffs):
        return [
            jnp.concatenate([lift(basis_t[c, r], coeffs) for r in range(rows)], axis=0)
            for c in range(comps)
        ]

    def inner(xs, ys):
        out = None
        for x, y in zip(xs, ys):
            out = x * y if out is None else out + x * y
        return out

    for load in small:
        load.wait()
    gram_full[my_col] = gram_ref[...]
    right = [r_ref[c] for c in range(comps)]
    free = [mask_ref[c].astype(F32) for c in range(comps)]
    visc = visc_ref[...]
    for d in EVERY:
        put_edge(0, d, [visc], 2 * comps if d < 2 else 2)
    for d in (NORTH, EAST):
        put_edge(0, d, right, 0)
        put_edge(0, d, free, comps if d < 2 else 1)

    row_copy = pltpu.make_async_remote_copy(
        src_ref=basis_t.at[:, rows - 1],
        dst_ref=row_recv,
        send_sem=row_ssem,
        recv_sem=row_rsem,
        device_id=where_to[NORTH],
        device_id_type=MESH,
    )
    col_copy = pltpu.make_async_remote_copy(
        src_ref=col_send,
        dst_ref=col_recv,
        send_sem=col_ssem,
        recv_sem=col_rsem,
        device_id=where_to[EAST],
        device_id_type=MESH,
    )

    def gram_copy(i):
        return pltpu.make_async_remote_copy(
            src_ref=gram_ref,
            dst_ref=gram_full.at[my_col],
            send_sem=gram_ssem,
            recv_sem=gram_rsem,
            device_id=(my_row, lax.rem(my_col + i, ncol)),
            device_id_type=MESH,
        )

    pl.semaphore_wait(barrier, greeted)
    tell_lower()
    send_edges(0, EVERY)
    pltpu.make_async_copy(basis_t, basis_t, load_sem).wait()
    keep_sums(0, total_row(project(right), []))

    pl.when(top)(lambda: send_sums(0))
    pl.when(has[NORTH])(row_copy.start)
    for i in range(1, ncol):
        gram_copy(i).start()

    column = jnp.zeros((basis, lanes), F32)
    for c in range(comps):
        for r in range(rows):
            spot = c * rows + r
            turned = pltpu.roll(basis_t[c, r], (spot + 1) % lanes, axis=1)
            column = jnp.where(wide_lane == spot, turned, column)
    col_send[...] = column
    pl.when(has[EAST])(col_copy.start)

    def send_plane(q):
        for dr in zigzag(depth) + [0]:
            row = q * depth + lax.rem(spot_row + dr, depth)
            for dc in zigzag(ncol) + [0]:
                send_to(0, (row, lax.rem(my_col + dc, ncol)))

    def hear_and_send():
        for dr in zigzag(depth) + [0]:
            row = plane * depth + lax.rem(spot_row + dr, depth)
            for dc in zigzag(ncol) + [0]:
                if dr or dc:
                    send_to(0, (row, lax.rem(my_col + dc, ncol)))
        for q in range(planes - 1):
            pl.when(q < plane)(functools.partial(send_plane, q))
        for q in range(1, planes):

            @pl.when(q > plane)
            def _(q=q):
                pl.semaphore_wait(chain_sem.at[q], 1)
                send_plane(q)

    pl.when(above)(hear_and_send)

    wait_edges(0, (EAST, WEST))
    sides = [row_to_cols(edge_recv[0, d, 2:3])[0] for d in (EAST, WEST)]
    _, below_visc, *beside = shifted(visc, 0.0, 0.0, *sides)
    open_north = 1.0 + 0.5 * (visc + below_visc)
    for v in beside:
        open_north = open_north + 0.5 * (visc + v)
    edge_send[1, NORTH, 0:1] = open_north[rows - 1 : rows]
    send_edges(1, (NORTH,))

    wait_edges(0, (NORTH, SOUTH))
    visc_halo = [edge_recv[0, d, 2 * comps : 2 * comps + 1] for d in (NORTH, SOUTH)]
    faces = [0.5 * (visc + v) for v in shifted(visc, *visc_halo, *sides)]
    diagonal = 1.0 + faces[0] + faces[1] + faces[2] + faces[3]
    inverse = 1.0 / diagonal
    scaled = [u * inverse for u in free]
    jacobi = [s + (1.0 - u) for s, u in zip(scaled, free)]
    put_edge(1, EAST, scaled, 0)
    send_edges(1, (EAST,))

    pl.when(has[SOUTH])(row_copy.wait_recv)
    pl.when(has[WEST])(col_copy.wait_recv)
    others = gram_full.at[pl.ds(0, ncol - 1)]
    pltpu.make_async_copy(others, others, gram_rsem).wait()
    gram = gram_full[...].reshape(basis, basis)
    wait_edges(1, (SOUTH, WEST))
    south_right = [edge_recv[0, SOUTH, c : c + 1] for c in range(comps)]
    south_free = [edge_recv[0, SOUTH, comps + c : comps + c + 1] for c in range(comps)]
    south_inverse = 1.0 / jnp.where(
        has[SOUTH], edge_recv[1, SOUTH, 0:1] + faces[1][0:1], 1.0
    )
    south_scaled = [u * south_inverse for u in south_free]
    west_right, west_free = edge_recv[0, WEST, 0:1], edge_recv[0, WEST, 1:2]
    west_scaled = edge_recv[1, WEST, 0:1]

    def halo_values(lifted, south_res, west_res):
        south = [
            a * r + u * b
            for a, r, u, b in zip(south_scaled, south_res, south_free, lifted[0])
        ]
        return south, west_scaled * west_res + west_free * lifted[1]

    def lift_halos(coeffs):
        south = [lift(row_recv[c], coeffs) for c in range(comps)]
        return south, lift(col_recv[...], coeffs)

    def operate(x, south, west):
        west_cols = row_to_cols(west)
        out, to_south, to_west = [], [], []
        for c in range(comps):
            masked = free[c] * x[c]
            around = shifted(masked, 0.0, south[c], 0.0, west_cols[c])
            stencil = diagonal * masked - (
                faces[0] * around[0]
                + faces[1] * around[1]
                + faces[2] * around[2]
                + faces[3] * around[3]
            )
            out.append(free[c] * stencil + (1.0 - free[c]) * x[c])
            to_south.append(faces[1] * masked)
            to_west.append(faces[3] * masked)
        return out, to_south, to_west

    def put_terms(stage, to_south, to_west):
        south_rows = edge_rows(SOUTH, to_south)
        west_row = edge_rows(WEST, to_west)[0]
        for c in range(comps):
            edge_send[stage, SOUTH, c : c + 1] = south_rows[c]
        edge_send[stage, WEST, 0:1] = west_row
        return [-u * q for u, q in zip(south_free, south_rows)], -west_free * west_row

    def cross(south, west, south_term, west_term):
        total = west * west_term
        for a, b in zip(south, south_term):
            total = total + a * b
        return jnp.where(row_of == 0, total, 0.0)

    def complete(stage, image):
        east_cols = row_to_cols(edge_recv[stage, EAST, 0:1])
        return [
            image[c]
            - free[c]
            * (
                jnp.where(row_of == rows - 1, edge_recv[stage, NORTH, c : c + 1], 0.0)
                + jnp.where(lane_of == lanes - 1, east_cols[c], 0.0)
            )
            for c in range(comps)
        ]

    def solve(dot):
        return jnp.sum(gram * dot[:, :basis], axis=1, keepdims=True) * scale

    dot = wait_sums(0)
    coeffs = solve(dot)
    lifted, lifted_halos = lift_all(coeffs), lift_halos(coeffs)
    direction = [j * r + b for j, r, b in zip(jacobi, right, lifted)]
    south, west = halo_values(lifted_halos, south_right, west_right)
    image, to_south, to_west = operate(direction, south, west)
    south_term, west_term = put_terms(2, to_south, to_west)
    across = project(image)
    extra = col_recv[...] * west_term
    for c in range(comps):
        extra = extra + row_recv[c] * south_term[c]
    across = [a + extra[i * rows : (i + 1) * rows] for i, a in enumerate(across)]
    second = total_row(
        across,
        [
            inner(right, direction),
            inner(direction, image) + cross(south, west, south_term, west_term),
        ],
    )
    keep_sums(1, second)
    send_sums(1)
    for d in (NORTH, EAST):
        put_edge(2, d, image, 0)
    corner_row = jnp.where(row_of == rows - 1, 1.0, 0.0)
    turned = [pltpu.roll(q, lanes - 1, axis=1) for q in to_west]
    for c in range(comps):
        diag_send[0, c : c + 1] = jnp.where(
            lane_of == lanes - 1, turned[c], 0.0
        )[rows - 1 : rows]
    turned = [pltpu.roll(q, rows - 1, axis=0) * corner_row for q in to_south]
    diag_send[1, 0:1] = col_to_row([q[:, lanes - 1 : lanes] for q in turned])
    send_edges(2, EVERY)
    for i in range(2):
        pl.when(has_diag[i])(diag_copy(i).start)
    wait_edges(2, EVERY)
    for i in range(2):
        pl.when(has_diag[1 - i])(diag_copy(i).wait_recv)
    image = complete(2, image)
    south_image = [
        edge_recv[2, SOUTH, c : c + 1]
        + south_term[c]
        - south_free[c] * diag_recv[0, c : c + 1]
        for c in range(comps)
    ]
    west_image = edge_recv[2, WEST, 0:1] + west_term - west_free * diag_recv[1, 0:1]
    sums = wait_sums(1)
    energy, curve = spread(sums, basis), spread(sums, basis + 1)
    step = energy / curve
    coeffs = solve(sums)
    residual = [r - step * w for r, w in zip(right, image)]
    smoothed = [
        j * r + (b - step * l)
        for j, r, b, l in zip(jacobi, residual, lifted, lift_all(coeffs))
    ]
    south_lift, west_lift = lift_halos(coeffs)
    south, west = halo_values(
        (
            [b - step * l for b, l in zip(lifted_halos[0], south_lift)],
            lifted_halos[1] - step * west_lift,
        ),
        [r - step * w for r, w in zip(south_right, south_image)],
        west_right - step * west_image,
    )
    smoothed_image, to_south, to_west = operate(smoothed, south, west)
    south_term, west_term = put_terms(3, to_south, to_west)
    third = total_row(
        [],
        [
            inner(residual, smoothed),
            inner(smoothed, image),
            inner(smoothed, smoothed_image)
            + cross(south, west, south_term, west_term),
        ],
    )
    keep_sums(2, third)
    send_sums(2)
    send_edges(3, (SOUTH, WEST))
    wait_edges(3, (NORTH, EAST))
    smoothed_image = complete(3, smoothed_image)
    for i in range(2):
        pl.when(has_diag[i])(diag_copy(i).wait_send)
    pl.when(has[NORTH])(row_copy.wait_send)
    pl.when(has[EAST])(col_copy.wait_send)
    pltpu.make_async_copy(others, others, gram_ssem).wait()
    sums = wait_sums(2)
    energy_new = spread(sums, 0)
    ratio = energy_new / energy
    curve_new = spread(sums, 2) + ratio * (2.0 * spread(sums, 1) + ratio * curve)
    step_new = energy_new / curve_new
    for c in range(comps):
        out_ref[c] = step * direction[c] + step_new * (smoothed[c] + ratio * direction[c])
        out_ref[comps + c] = residual[c] - step_new * (smoothed_image[c] + ratio * image[c])

    drain_sums()
    drain_edges()


def on_device(nrow, ncol, right_side, viscosity, free_mask, coarse_basis, gram_inverse):
    comps, rows, lanes = right_side.shape
    basis = coarse_basis.shape[0]
    n = nrow * ncol
    unknowns = comps * rows * lanes * n * basis
    scale = 1.0 / (32.0 * math.sqrt(float(unknowns)))
    vmem = pl.BlockSpec(memory_space=pltpu.VMEM)
    dma = pltpu.SemaphoreType.DMA
    out = pl.pallas_call(
        functools.partial(kernel, nrow, ncol, scale),
        out_shape=pltpu.VMEM((2 * comps, rows, lanes), F32),
        in_specs=[pl.BlockSpec(memory_space=pltpu.HBM)] * 5,
        out_specs=vmem,
        scratch_shapes=[
            pltpu.VMEM(right_side.shape, F32),
            pltpu.VMEM(viscosity.shape, F32),
            pltpu.VMEM(free_mask.shape, free_mask.dtype),
            pltpu.VMEM(gram_inverse.shape, F32),
            pltpu.VMEM((comps, rows, basis, lanes), F32),
            pltpu.VMEM((comps, basis, lanes), F32),
            pltpu.VMEM((basis, lanes), F32),
            pltpu.VMEM((basis, lanes), F32),
            pltpu.VMEM((4, 4, 8, lanes), F32),
            pltpu.VMEM((4, 4, 8, lanes), F32),
            pltpu.VMEM((2, 8, lanes), F32),
            pltpu.VMEM((2, 8, lanes), F32),
            pltpu.VMEM((ncol,) + gram_inverse.shape, F32),
            pltpu.VMEM((3, 1, lanes), F32),
            pltpu.VMEM((3, n, 1, lanes), F32),
            dma,
            dma((4,)),
            dma,
            dma,
            dma,
            dma,
            dma((4,)),
            dma((len(SENT_AT),)),
            dma((2,)),
            dma((2,)),
            dma,
            dma,
            dma,
            dma((3,)),
            pltpu.SemaphoreType.REGULAR((nrow // plane_rows(nrow),)),
        ],
        compiler_params=pltpu.CompilerParams(
            collective_id=0, has_side_effects=True, vmem_limit_bytes=60_000_000
        ),
    )(right_side, viscosity, free_mask, coarse_basis, gram_inverse)
    return out[:comps], out[comps:]


def solution(mesh):
    in_specs = (
        P(None, "row", "col"),
        P("row", "col"),
        P(None, "row", "col"),
        P(None, None, "row", "col"),
        P("col", None),
    )
    out_specs = (P(None, "row", "col"), P(None, "row", "col"))
    return jax.shard_map(
        functools.partial(on_device, mesh.shape["row"], mesh.shape["col"]),
        mesh=mesh,
        in_specs=in_specs,
        out_specs=out_specs,
        check_vma=False,
    )
```
